32 devices in a mesh: mem: 8 (over z, x), blk: 4 (over y, core).
Axes of the slice: x: 2, y: 2, z: 4, core: 2. Of those that a mesh axis runs over, the one named last changes fastest.
Arguments:
- ensemble: bfloat16 [128, 131072], P('mem', 'blk'), may hold values from -6 to 6
- obs_cell: int32 [4, 64, 256], P('blk', 'mem'), may hold values from 0 to 511
- obs_count: int32 [4, 64], P('blk', 'mem'), may hold values from 1 to 256, 10240 in all within a row
- obs_value: float32 [4, 64, 256], P('blk', 'mem'), may hold values from -6 to 6
- obs_rinv: float32 [4, 64, 256], P('blk', 'mem'), may hold values from 0.05 to 0.5
Outputs:
- increments: bfloat16 [128, 131072], P('mem', 'blk')
The draws below stay inside these ranges and needn't reach their ends.
Inputs may be any that keep to these rules, and one draw needn't show every extreme that they name: `obs_cell`: slots at or past the block's count are unused. `obs_count`: the counts of one band sum to 10240, and some block holds exactly 256.
All inputs are finite; a program needn't handle non-finite values. Where the reference program divides by a largest or mean magnitude, that divisor is 1e-20 or more.
Results may differ from the reference program's by a relative error of at most 0.0051.
Values may be sent and summed in bfloat16 or wider, within the bound.
A program may use at most 64 MiB of HBM per device.

```python
import math
import jax
import jax.numpy as jnp
import numpy as np
from jax import lax

K = 128
CELLS = 512
OMAX = 256
NS_ITERS = 4
NSB = 64
CELLS_ALL = 131072
N_BLK = 4


def place_ends(array, key, least, top_value):
    shape = array.shape
    index_at = [jax.random.randint(jax.random.fold_in(key, axis), (), 0, shape[axis]) for axis in range(len(shape))]
    array = array.at[tuple(index_at)].set(least)
    longest = shape.index(max(shape))
    index_at[longest] = (index_at[longest] + 1) % shape[longest]
    return array.at[tuple(index_at)].set(top_value)


def block_scale(key, dims, pieces, smallest, largest):
    loudness, own = 1.0, jax.random.fold_in(key, 6)
    for dim, blocks in pieces:
        draws = jnp.exp(jax.random.uniform(jax.random.fold_in(own, dim), (blocks,), jnp.float32, smallest / len(pieces), largest / len(pieces)))
        loudness = loudness * jnp.repeat(draws, dims[dim] // blocks).reshape([-1 if axis == dim else 1 for axis in range(len(dims))])
    return loudness


def length_profile(count, total, limit, lean):
    portions = [(1 << 20) // math.isqrt(grade ** lean) + 1 for grade in range(2, count + 1)]
    rest, counts = total - limit - (count - 1), [1] * (count - 1)
    while rest > 0:
        movable = [i for i in range(count - 1) if counts[i] < limit]
        mass, remaining = sum([portions[i] for i in movable]), rest
        for i in movable:
            extra = min(limit - counts[i], max(1, remaining * portions[i] // mass), rest)
            counts[i] = counts[i] + extra
            rest = rest - extra
    return np.array([limit] + counts)


def uneven(stream_key, count, total, most, lean):
    if count == 2:
        one = jax.random.randint(stream_key, (), max(1, total - most), min(most, total - 1) + 1)
        return jnp.stack([one, total - one])
    sizes = jnp.asarray(length_profile(count, total, most, lean), jnp.int32)
    pairs = (count - 1) // 2
    giver, receiver = sizes[1:1 + 2 * pairs:2], sizes[2:2 + 2 * pairs:2]
    margin = jnp.minimum(giver - 1, most - receiver)
    passed = jax.random.randint(jax.random.fold_in(stream_key, 1), (pairs,), 0, 1 << 20) % (margin + 1)
    sizes = sizes.at[1:1 + 2 * pairs:2].set(giver - passed).at[2:2 + 2 * pairs:2].set(receiver + passed)
    return sizes[jax.random.permutation(jax.random.fold_in(stream_key, 2), count)]


def bell_draw(own_key, shape, scale, bound, split=(), kind=jnp.bfloat16):
    array = jax.random.normal(own_key, shape, jnp.float32) * scale
    if len(split) > 0:
        array = block_scale(own_key, shape, split, -0.22, 0.18) * array
    return jnp.clip(array, min=-bound, max=bound).astype(kind)


def setup_inputs(seed: int = 0) -> dict:
    seeds = jax.random.split(jax.random.key(seed), 6)
    ensemble = bell_draw(seeds[0], (K, CELLS_ALL), 1.0, 6.0, ((0, 8), (1, 4)))
    obs_cell = place_ends(jax.random.randint(seeds[1], (N_BLK, NSB, OMAX), 0, CELLS), jax.random.fold_in(seeds[1], 1), 0, CELLS - 1).astype(jnp.int32)
    obs_count = jax.vmap(lambda own: uneven(own, NSB, NSB * OMAX * 5 // 8, OMAX, 2))(jax.random.split(seeds[2], N_BLK)).reshape((N_BLK, NSB)).astype(jnp.int32)
    obs_value = bell_draw(seeds[3], (N_BLK, NSB, OMAX), 1.0, 6.0, ((0, 4), (1, 8)), jnp.float32)
    obs_rinv = jnp.clip(jnp.exp(math.log(0.5) - 2.3025851 * jax.random.uniform(seeds[4], (N_BLK, NSB, OMAX), jnp.float32) ** block_scale(seeds[4], (N_BLK, NSB, OMAX), ((0, 4), (1, 8)), -0.2, 0.2)), 0.05, 0.5)
    return {"ensemble": ensemble, "obs_cell": obs_cell, "obs_count": obs_count, "obs_value": obs_value, "obs_rinv": obs_rinv}


localize = 0.5
inflation = 1.1

def center(members):
    values = members.astype(jnp.float32)
    average = lax.optimization_barrier(jnp.mean(values, axis=0))
    return (values - average[None], average)

def observe(deviation, average, cell_ids, live_counts, obs_values, inv_var):
    ensemble_size = deviation.shape[0]
    index = jnp.broadcast_to(cell_ids[None].astype(jnp.int32), (ensemble_size,) + cell_ids.shape)
    sampled = jnp.take_along_axis(deviation, index, axis=2)
    obs_mean = jnp.take_along_axis(average, cell_ids.astype(jnp.int32), axis=1)
    slots = lax.broadcasted_iota(jnp.int32, cell_ids.shape, 1)
    live = (slots < live_counts[:, None].astype(jnp.int32)).astype(jnp.float32)
    weight_root = live * jnp.sqrt(inv_var)
    upper = jnp.transpose(sampled * weight_root[None], (1, 0, 2))
    lower = (weight_root * (obs_values - obs_mean))[:, None, :]
    return jnp.concatenate([upper, lower], axis=1).astype(jnp.bfloat16)

def batch_mm(left, right):
    return jnp.einsum('bij,bjk->bik', left, right, precision=lax.Precision.HIGHEST)

def transform_apply(localized, deviation):
    ensemble_size = deviation.shape[0]
    identity = jnp.eye(ensemble_size, dtype=jnp.float32)
    system = (ensemble_size - 1) / inflation * identity + localized[:, :ensemble_size, :ensemble_size]
    forcing = localized[:, :ensemble_size, ensemble_size]
    bound_norm = lax.optimization_barrier(jnp.max(lax.optimization_barrier(jnp.sum(jnp.abs(system), axis=2)), axis=1))
    approx_y = system / bound_norm[:, None, None]
    approx_z = jnp.broadcast_to(identity, system.shape)
    for iteration in range(NS_ITERS):
        update = 1.5 * identity - 0.5 * batch_mm(approx_z, approx_y)
        approx_y = batch_mm(approx_y, update)
        approx_z = batch_mm(update, approx_z)
    root_inv = approx_z / jnp.sqrt(bound_norm)[:, None, None]
    inner = jnp.einsum('bij,bj->bi', root_inv, forcing, precision=lax.Precision.HIGHEST)
    mean_weights = jnp.einsum('bij,bj->bi', root_inv, inner, precision=lax.Precision.HIGHEST)
    mixing = jnp.sqrt(jnp.float32(ensemble_size - 1)) * root_inv + mean_weights[:, :, None] - identity
    increment = jnp.einsum('jbc,bjk->kbc', deviation, mixing, precision=lax.Precision.HIGHEST)
    return increment.astype(jnp.bfloat16)

def reference(ensemble, obs_cell, obs_count, obs_value, obs_rinv):
    bands = obs_cell.shape[0]
    sectors = obs_cell.shape[1]
    grid = jnp.transpose(ensemble.reshape(K, bands, sectors, CELLS), (1, 0, 2, 3))

    def one_band(band_inputs):
        members, cell_ids, live_counts, obs_values, inv_var = band_inputs
        deviation, average = center(members)
        obs_rows = observe(deviation, average, cell_ids, live_counts, obs_values, inv_var)
        wide_rows = obs_rows.astype(jnp.float32)
        gram_blocks = jnp.einsum('bko,bjo->bkj', wide_rows, wide_rows, precision=lax.Precision.HIGHEST)
        localized = gram_blocks + localize * (jnp.roll(gram_blocks, 1, axis=0) + jnp.roll(gram_blocks, -1, axis=0))
        return transform_apply(localized, deviation)
    result = lax.map(one_band, (grid, obs_cell, obs_count, obs_value, obs_rinv))
    return jnp.transpose(result, (1, 0, 2, 3)).reshape(K, bands * sectors * CELLS)
```

```python
import functools

import jax
import jax.numpy as jnp
from jax import lax
from jax.experimental import pallas as pl
from jax.experimental.pallas import tpu as pltpu
from jax.sharding import PartitionSpec as P

NS_ITERS = 4


localize = 0.5
inflation = 1.1

MESH = pl.DeviceIdType.MESH
CHUNK = 1
HELD_BACK = 2
F32 = jnp.float32
BF16 = jnp.bfloat16


def halves(x):
    high = x.astype(BF16)
    return high, (x - high.astype(F32)).astype(BF16)


def as_left(x):
    return jnp.concatenate(halves(x), axis=1)


def as_right(x):
    wide = jnp.concatenate(halves(x), axis=1)
    return jnp.concatenate([wide, wide], axis=0)


def mm(left, right):
    both = jnp.dot(left, right, preferred_element_type=F32)
    size = both.shape[1] // 2
    return both[:, :size] + both[:, size:]


def observed_rows(members, selector, values, root):
    ensemble_size = members.shape[0]
    sampled = jnp.dot(members, selector, preferred_element_type=F32)
    obs_mean = jnp.sum(sampled, axis=0, keepdims=True) * (1.0 / ensemble_size)
    upper = ((sampled - obs_mean) * root).astype(BF16)
    lower = root * (values - obs_mean)
    place = lax.broadcasted_iota(jnp.int32, (16, lower.shape[1]), 0)
    lower = jnp.where(place == 0, jnp.broadcast_to(lower, place.shape), 0.0).astype(BF16)
    return jnp.concatenate([upper, lower], axis=0)


def increments_of(localized, members):
    ensemble_size = members[0].shape[0]
    row = lax.broadcasted_iota(jnp.int32, (ensemble_size, ensemble_size), 0)
    column = lax.broadcasted_iota(jnp.int32, (ensemble_size, ensemble_size), 1)
    identity = (row == column).astype(F32)
    system = [
        (ensemble_size - 1) / inflation * identity + part[:ensemble_size] for part in localized
    ]
    bound_norm = [
        jnp.max(jnp.sum(jnp.abs(part), axis=0, keepdims=True), axis=1, keepdims=True)
        for part in system
    ]
    approx_y = [part / norm for part, norm in zip(system, bound_norm)]
    update = [1.5 * identity - 0.5 * part for part in approx_y]
    approx_z = update
    for iteration in range(1, NS_ITERS):
        approx_y = [mm(as_left(y), as_right(u)) for y, u in zip(approx_y, update)]
        left_z = [as_left(z) for z in approx_z]
        update = [
            1.5 * identity - 0.5 * mm(z, as_right(y)) for z, y in zip(left_z, approx_y)
        ]
        approx_z = [mm(z, as_right(u)) for z, u in zip(left_z, update)]
    root_inv = [z / jnp.sqrt(norm) for z, norm in zip(approx_z, bound_norm)]
    right_r = [as_right(part) for part in root_inv]
    inner = [mm(as_left(part[ensemble_size:]), r) for part, r in zip(localized, right_r)]
    mean_weights = [mm(as_left(part), r)[0:1] for part, r in zip(inner, right_r)]
    mixing = [
        jnp.sqrt(F32(ensemble_size - 1)) * part + weights - identity
        for part, weights in zip(root_inv, mean_weights)
    ]
    results = []
    for mixed, block in zip(mixing, members):
        high, low = halves(mixed)
        row_sum = jnp.sum(high.astype(F32) + low.astype(F32), axis=1, keepdims=True)
        average = jnp.sum(block.astype(F32), axis=0, keepdims=True) * (1.0 / ensemble_size)
        total = jnp.dot(
            jnp.concatenate([high, low], axis=1),
            jnp.concatenate([block, block], axis=0),
            preferred_element_type=F32,
        )
        results.append((total - row_sum * average).astype(BF16))
    return results


def kernel(
    groups,
    ens_hbm,
    cell_hbm,
    count_hbm,
    value_hbm,
    rinv_hbm,
    out,
    arrived,
    rows,
    gram,
    edge,
    far_edge,
    selector,
    stage,
    weight,
    cell,
    count,
    value,
    rinv,
    load_sem,
    own_sem,
    fwd_send,
    fwd_recv,
    ret_send,
    ret_recv,
    halo_send,
    halo_recv,
):
    me = lax.axis_index("mem")
    blocks, _, width = arrived.shape
    local = ens_hbm.shape[0]
    slots = cell.shape[1]
    size = groups * local

    barrier = pltpu.get_barrier_semaphore()
    for step in range(1, groups):
        pl.semaphore_signal(
            barrier, inc=1, device_id={"mem": lax.rem(me + step, groups)}, device_id_type=MESH
        )

    loads = [
        pltpu.make_async_copy(source, target, load_sem.at[i])
        for i, (source, target) in enumerate(
            ((cell_hbm, cell), (count_hbm, count), (value_hbm, value), (rinv_hbm, rinv))
        )
    ]
    for load in loads:
        load.start()
    pl.semaphore_wait(barrier, groups - 1)

    def columns(owner, b):
        start = pl.multiple_of((owner * blocks + b) * width, width)
        return pl.ds(start, width)

    def members_of(owner):
        return pl.ds(pl.multiple_of(owner * local, local), local)

    order = [blocks - 1, *range(blocks - 1)]
    for first in range(0, blocks, CHUNK):
        for step in range(1, groups):
            peer = lax.rem(me + step, groups)
            for b in order[first : first + CHUNK]:
                pltpu.make_async_remote_copy(
                    src_ref=ens_hbm.at[:, columns(peer, b)],
                    dst_ref=arrived.at[b, members_of(me), :],
                    send_sem=fwd_send,
                    recv_sem=fwd_recv.at[b],
                    device_id={"mem": peer},
                    device_id_type=MESH,
                ).start()
    for b in order:
        pltpu.make_async_copy(
            ens_hbm.at[:, columns(me, b)], arrived.at[b, members_of(me), :], fwd_recv.at[b]
        ).start()

    for load in loads:
        load.wait()
    weight[...] = jnp.sqrt(rinv[...])

    @pl.loop(0, blocks)
    def _(b):
        positions = lax.broadcasted_iota(jnp.int32, (width, slots), 0)
        selector[b] = jnp.where(positions == cell[pl.ds(b, 1), :], 1.0, 0.0).astype(BF16)

    def take_block(b):
        pltpu.make_async_copy(arrived.at[b], arrived.at[b], fwd_recv.at[b]).wait()
        alive = lax.broadcasted_iota(jnp.int32, (1, slots), 1) < count[0, b]
        root = jnp.where(alive, weight[pl.ds(b, 1), :], 0.0)
        held = observed_rows(arrived[b], selector[b], value[pl.ds(b, 1), :], root)
        rows[b] = held
        gram[b + 1] = lax.dot_general(
            held, held[:size], (((1,), (1,)), ((), ())), preferred_element_type=F32
        )

    def solve(pair):
        localized = [gram[b + 1] + localize * (gram[b] + gram[b + 2]) for b in pair]
        results = increments_of(localized, [arrived[b] for b in pair])
        for b, result in zip(pair, results):
            stage[b] = result

    def give_back(group):
        for step in range(1, groups):
            peer = lax.rem(me + step, groups)
            for b in group:
                pltpu.make_async_remote_copy(
                    src_ref=stage.at[b, members_of(peer), :],
                    dst_ref=out.at[:, columns(me, b)],
                    send_sem=ret_send,
                    recv_sem=ret_recv,
                    device_id={"mem": peer},
                    device_id_type=MESH,
                ).start()
        for b in group:
            pltpu.make_async_copy(
                stage.at[b, members_of(me), :], out.at[:, columns(me, b)], own_sem
            ).start()

    def halo(slot, peer, which):
        edge[which] = gram[slot].astype(BF16)
        return pltpu.make_async_remote_copy(
            src_ref=edge.at[which],
            dst_ref=far_edge.at[which],
            send_sem=halo_send.at[which],
            recv_sem=halo_recv.at[which],
            device_id={"mem": peer},
            device_id_type=MESH,
        )

    take_block(blocks - 1)
    upward = halo(blocks, lax.rem(me + 1, groups), 0)
    upward.start()
    take_block(0)
    downward = halo(1, lax.rem(me + groups - 1, groups), 1)
    downward.start()

    take_block(1)
    pairs = blocks // 2

    @pl.loop(0, pairs)
    def _(turn):
        b = 2 * turn + 1

        @pl.when(turn < pairs - 1)
        def _():
            @pl.loop(b + 1, jnp.minimum(b + 3, blocks - 1))
            def _(later):
                take_block(later)

        @pl.when(turn == pairs - 1)
        def _():
            upward.wait_recv()
            gram[0] = far_edge[0].astype(F32)
            downward.wait_recv()
            gram[blocks + 1] = far_edge[1].astype(F32)

        final = turn == pairs - 1
        solve([jnp.where(final, 0, b), jnp.where(final, blocks - 1, b + 1)])

        for i in range(pairs - HELD_BACK):
            @pl.when(turn == i)
            def _():
                give_back([2 * i + 1, 2 * i + 2])

    held_back = [*range(2 * (pairs - HELD_BACK) + 1, blocks), 0]
    give_back(held_back)

    upward.wait_send()
    downward.wait_send()
    share = blocks * width
    afar = pl.ds(0, (groups - 1) * share)
    pltpu.make_async_copy(out.at[:, afar], out.at[:, afar], fwd_send).wait()
    pltpu.make_async_copy(out.at[:, afar], out.at[:, afar], ret_send).wait()
    pltpu.make_async_copy(out.at[:, afar], out.at[:, afar], ret_recv).wait()
    near = pl.ds(0, share)
    pltpu.make_async_copy(out.at[:, near], out.at[:, near], own_sem).wait()


def fused(ensemble, obs_cell, obs_count, obs_value, obs_rinv):
    groups = lax.axis_size("mem")
    local, cells = ensemble.shape
    blocks, slots = obs_cell.shape[1:]
    width = cells // (groups * blocks)
    size = groups * local
    whole = pl.BlockSpec(memory_space=pltpu.VMEM)
    return pl.pallas_call(
        functools.partial(kernel, groups),
        out_shape=pltpu.VMEM(ensemble.shape, BF16),
        in_specs=[pl.BlockSpec(memory_space=pl.ANY)] * 5,
        out_specs=whole,
        scratch_shapes=[
            pltpu.VMEM((blocks, size, width), BF16),
            pltpu.VMEM((blocks, size + 16, slots), BF16),
            pltpu.VMEM((blocks + 2, size + 16, size), F32),
            pltpu.VMEM((2, size + 16, size), BF16),
            pltpu.VMEM((2, size + 16, size), BF16),
            pltpu.VMEM((blocks, width, slots), BF16),
            pltpu.VMEM((blocks, size, width), BF16),
            pltpu.VMEM((blocks, slots), F32),
            pltpu.VMEM((blocks, slots), jnp.int32),
            pltpu.SMEM(obs_count.shape, jnp.int32),
            pltpu.VMEM((blocks, slots), F32),
            pltpu.VMEM((blocks, slots), F32),
            pltpu.SemaphoreType.DMA((4,)),
            pltpu.SemaphoreType.DMA,
            pltpu.SemaphoreType.DMA,
            pltpu.SemaphoreType.DMA((blocks,)),
            pltpu.SemaphoreType.DMA,
            pltpu.SemaphoreType.DMA,
            pltpu.SemaphoreType.DMA((2,)),
            pltpu.SemaphoreType.DMA((2,)),
        ],
        compiler_params=pltpu.CompilerParams(collective_id=0, has_side_effects=True),
        name="letkf",
    )(ensemble, obs_cell[0], obs_count, obs_value[0], obs_rinv[0])


def with_halo(block, sides, width):
    for axis, dim in sides:
        count = lax.axis_size(axis)
        forward = [(i, i + 1) for i in range(count - 1)]
        forward.append((count - 1, 0))
        backward = [(target, source) for source, target in forward]
        low = lax.ppermute(
            lax.slice_in_dim(block, block.shape[dim] - width, None, axis=dim), axis, forward
        )
        high = lax.ppermute(lax.slice_in_dim(block, 0, width, axis=dim), axis, backward)
        block = jnp.concatenate([low, block, high], axis=dim)
    return block


def center_blocks(members):
    values = jnp.transpose(members.astype(jnp.float32), (1, 0, 2))
    average = jnp.mean(values, axis=1)
    return (values - average[:, None, :], average)


def observe(deviation, average, cell_ids, live_counts, obs_values, inv_var):
    cell_width = deviation.shape[2]
    positions = lax.broadcasted_iota(jnp.int32, cell_ids.shape + (cell_width,), 2)
    selector = (positions == cell_ids[:, :, None]).astype(jnp.float32)
    sampled = jnp.einsum("bkc,boc->bko", deviation, selector, precision=lax.Precision.HIGHEST)
    obs_mean = jnp.einsum("bc,boc->bo", average, selector, precision=lax.Precision.HIGHEST)
    slots = lax.broadcasted_iota(jnp.int32, cell_ids.shape, 1)
    live = (slots < live_counts[:, None]).astype(jnp.float32)
    weight_root = live * jnp.sqrt(inv_var)
    upper = sampled * weight_root[:, None, :]
    lower = (weight_root * (obs_values - obs_mean))[:, None, :]
    return jnp.concatenate([upper, lower], axis=1).astype(jnp.bfloat16)


def gram_of(obs_rows):
    return jnp.einsum("bko,bjo->bkj", obs_rows, obs_rows, preferred_element_type=jnp.float32)


def batch_mm(left, right):
    return jnp.einsum("bij,bjk->bik", left, right, precision=lax.Precision.HIGHEST)


def transform_apply(localized, deviation):
    ensemble_size = deviation.shape[1]
    identity = jnp.eye(ensemble_size, dtype=jnp.float32)
    system = (ensemble_size - 1) / inflation * identity + localized[
        :, :ensemble_size, :ensemble_size
    ]
    forcing = localized[:, :ensemble_size, ensemble_size]
    bound_norm = jnp.max(jnp.sum(jnp.abs(system), axis=2), axis=1)
    approx_y = system / bound_norm[:, None, None]
    approx_z = jnp.broadcast_to(identity, system.shape)
    for iteration in range(NS_ITERS):
        update = 1.5 * identity - 0.5 * batch_mm(approx_z, approx_y)
        approx_y = batch_mm(approx_y, update)
        approx_z = batch_mm(update, approx_z)
    root_inv = approx_z / jnp.sqrt(bound_norm)[:, None, None]
    inner = jnp.einsum("bij,bj->bi", root_inv, forcing, precision=lax.Precision.HIGHEST)
    mean_weights = jnp.einsum("bij,bj->bi", root_inv, inner, precision=lax.Precision.HIGHEST)
    mixing = (
        jnp.sqrt(jnp.float32(ensemble_size - 1)) * root_inv + mean_weights[:, :, None] - identity
    )
    increment = jnp.einsum("bjc,bjk->kbc", deviation, mixing, precision=lax.Precision.HIGHEST)
    return increment.astype(jnp.bfloat16)


def on_device(ensemble, obs_cell, obs_count, obs_value, obs_rinv):
    groups = lax.axis_size("mem")
    local_members = ensemble.shape[0]
    blocks = obs_cell.shape[1]
    cell_width = ensemble.shape[1] // (groups * blocks)
    pieces = ensemble.reshape(local_members, groups, blocks, cell_width)
    arrived = lax.all_to_all(pieces, "mem", split_axis=1, concat_axis=0, tiled=True)
    deviation, average = center_blocks(arrived[:, 0])
    obs_rows = observe(deviation, average, obs_cell[0], obs_count[0], obs_value[0], obs_rinv[0])
    padded_rows = with_halo(obs_rows, (("mem", 0),), 1)
    padded = gram_of(padded_rows)
    localized = padded[1:-1] + localize * (padded[:-2] + padded[2:])
    increment = transform_apply(localized, deviation)
    ensemble_size = increment.shape[0]
    outgoing = increment.reshape(ensemble_size, 1, blocks * cell_width)
    returned = lax.all_to_all(outgoing, "mem", split_axis=0, concat_axis=1, tiled=True)
    return returned.reshape(local_members, groups * blocks * cell_width)


def by_shape(ensemble, *observations):
    groups = lax.axis_size("mem")
    local, cells = ensemble.shape
    blocks, slots = observations[0].shape[1:]
    width = cells // (groups * blocks)
    aligned = local % 16 == 0 and width % 128 == 0 and slots % 128 == 0
    aligned = aligned and (groups * local) % 128 == 0 and groups > 1 and blocks > 2 and blocks % 2 == 0
    return (fused if aligned else on_device)(ensemble, *observations)


def solution(mesh):
    placed = (
        P("mem", "blk"),
        P("blk", "mem", None),
        P("blk", "mem"),
        P("blk", "mem", None),
        P("blk", "mem", None),
    )
    return jax.shard_map(
        by_shape, mesh=mesh, in_specs=placed, out_specs=P("mem", "blk"), check_vma=False
    )
```

```python
import functools

import jax
import jax.numpy as jnp
from jax import lax
from jax.experimental import pallas as pl
from jax.experimental.pallas import tpu as pltpu
from jax.sharding import PartitionSpec as P

NS_ITERS = 4


localize = 0.5
inflation = 1.1

MESH = pl.DeviceIdType.MESH
HELD_BACK = 2
EARLY_INNER = 4
EARLY_OUTER = 3
F32 = jnp.float32
BF16 = jnp.bfloat16


def halves(x):
    high = x.astype(BF16)
    return high, (x - high.astype(F32)).astype(BF16)


def as_left(x):
    return jnp.concatenate(halves(x), axis=1)


def as_right(x):
    wide = jnp.concatenate(halves(x), axis=1)
    return jnp.concatenate([wide, wide], axis=0)


def mm(left, right):
    both = jnp.dot(left, right, preferred_element_type=F32)
    size = both.shape[1] // 2
    return both[:, :size] + both[:, size:]


def observed_rows(members, selector, values, root):
    ensemble_size = members.shape[0]
    sampled = jnp.dot(members, selector, preferred_element_type=F32)
    obs_mean = jnp.sum(sampled, axis=0, keepdims=True) * (1.0 / ensemble_size)
    upper = ((sampled - obs_mean) * root).astype(BF16)
    lower = root * (values - obs_mean)
    place = lax.broadcasted_iota(jnp.int32, (16, lower.shape[1]), 0)
    lower = jnp.where(place == 0, jnp.broadcast_to(lower, place.shape), 0.0).astype(BF16)
    return jnp.concatenate([upper, lower], axis=0)


def increments_of(localized, members):
    ensemble_size = members[0].shape[0]
    row = lax.broadcasted_iota(jnp.int32, (ensemble_size, ensemble_size), 0)
    column = lax.broadcasted_iota(jnp.int32, (ensemble_size, ensemble_size), 1)
    identity = (row == column).astype(F32)
    system = [
        (ensemble_size - 1) / inflation * identity + part[:ensemble_size] for part in localized
    ]
    bound_norm = [
        jnp.max(jnp.sum(jnp.abs(part), axis=0, keepdims=True), axis=1, keepdims=True)
        for part in system
    ]
    approx_y = [part / norm for part, norm in zip(system, bound_norm)]
    update = [1.5 * identity - 0.5 * part for part in approx_y]
    approx_z = update
    for iteration in range(1, NS_ITERS):
        approx_y = [mm(as_left(y), as_right(u)) for y, u in zip(approx_y, update)]
        left_z = [as_left(z) for z in approx_z]
        update = [
            1.5 * identity - 0.5 * mm(z, as_right(y)) for z, y in zip(left_z, approx_y)
        ]
        approx_z = [mm(z, as_right(u)) for z, u in zip(left_z, update)]
    root_inv = [z / jnp.sqrt(norm) for z, norm in zip(approx_z, bound_norm)]
    right_r = [as_right(part) for part in root_inv]
    inner = [mm(as_left(part[ensemble_size:]), r) for part, r in zip(localized, right_r)]
    mean_weights = [mm(as_left(part), r)[0:1] for part, r in zip(inner, right_r)]
    mixing = [
        jnp.sqrt(F32(ensemble_size - 1)) * part + weights - identity
        for part, weights in zip(root_inv, mean_weights)
    ]
    results = []
    for mixed, block in zip(mixing, members):
        high, low = halves(mixed)
        row_sum = jnp.sum(high.astype(F32) + low.astype(F32), axis=1, keepdims=True)
        average = jnp.sum(block.astype(F32), axis=0, keepdims=True) * (1.0 / ensemble_size)
        total = jnp.dot(
            jnp.concatenate([high, low], axis=1),
            jnp.concatenate([block, block], axis=0),
            preferred_element_type=F32,
        )
        results.append((total - row_sum * average).astype(BF16))
    return results


def kernel(
    groups,
    ens_hbm,
    cell_hbm,
    count_hbm,
    value_hbm,
    rinv_hbm,
    out,
    arrived,
    rows,
    gram,
    edge,
    far_edge,
    selector,
    stage,
    weight,
    cell,
    count,
    value,
    rinv,
    load_sem,
    own_sem,
    fwd_send,
    fwd_recv,
    ret_send,
    ret_recv,
    halo_send,
    halo_recv,
    joined,
    told,
    spread,
    complete,
):
    me = lax.axis_index("mem")
    blocks, _, width = arrived.shape
    local = ens_hbm.shape[0]
    slots = cell.shape[1]
    size = groups * local

    lanes = 2
    spots = groups // lanes
    split = groups > 2 * lanes and groups % (2 * lanes) == 0

    def central(peer):
        spot = peer // lanes
        return (spot == spots // 2 - 1) | (spot == spots // 2)

    def notify(semaphore, peer):
        pl.semaphore_signal(semaphore, inc=1, device_id={"mem": peer}, device_id_type=MESH)

    others = [lax.rem(me + step, groups) for step in range(1, groups)]
    barrier = pltpu.get_barrier_semaphore()
    if split:
        inner = central(me)
        outer = jnp.logical_not(inner)
        upper = me // lanes >= spots // 2
        lane = lax.rem(me, lanes)
        parent = (spots // 2 - 1 + upper.astype(jnp.int32)) * lanes + lane
        first = jnp.where(upper, spots // 2 + 1, 0) * lanes + lane
        children = [first + i * lanes for i in range(spots // 2 - 1)]

        def to_central(semaphore):
            for peer in others:
                pl.when(central(peer))(lambda: notify(semaphore, peer))

        def to_children(semaphore):
            for child in children:
                notify(semaphore, child)

        @pl.when(inner)
        def _():
            to_central(barrier)
            to_children(barrier)
    else:
        for peer in others:
            notify(barrier, peer)

    loads = [
        pltpu.make_async_copy(source, target, load_sem.at[i])
        for i, (source, target) in enumerate(
            ((cell_hbm, cell), (count_hbm, count), (value_hbm, value), (rinv_hbm, rinv))
        )
    ]
    for load in loads:
        load.start()
    if split:
        pl.semaphore_wait(barrier, jnp.where(inner, 2 * lanes - 1, 1))
    else:
        pl.semaphore_wait(barrier, groups - 1)

    def columns(owner, b):
        start = pl.multiple_of((owner * blocks + b) * width, width)
        return pl.ds(start, width)

    def members_of(owner):
        return pl.ds(pl.multiple_of(owner * local, local), local)

    order = [blocks - 1, *range(blocks - 1)]
    def send_to(b, peer):
        pltpu.make_async_remote_copy(
            src_ref=ens_hbm.at[:, columns(peer, b)],
            dst_ref=arrived.at[b, members_of(me), :],
            send_sem=fwd_send,
            recv_sem=fwd_recv.at[b],
            device_id={"mem": peer},
            device_id_type=MESH,
        ).start()

    def send_where(wanted, chosen):
        for b in chosen:
            for peer in others:
                pl.when(wanted(peer))(lambda: send_to(b, peer))

    def send_all(chosen):
        for b in chosen:
            for peer in others:
                send_to(b, peer)

    def beyond(peer):
        return jnp.logical_not(central(peer))

    if split:

        @pl.when(inner)
        def _():
            send_where(central, order[:EARLY_INNER])
            pl.semaphore_wait(joined, len(children))
            to_children(told)
            to_central(spread)
            pl.semaphore_wait(spread, 2 * lanes - 1)
            to_children(complete)
            send_where(beyond, order[:EARLY_INNER])
            send_all(order[EARLY_INNER:])

        @pl.when(outer)
        def _():
            notify(joined, parent)
            pl.semaphore_wait(told, 1)
            send_where(central, order[:EARLY_OUTER])
            pl.semaphore_wait(complete, 1)
            send_where(beyond, order[:EARLY_OUTER])
            send_all(order[EARLY_OUTER:])
    else:
        send_all(order)

    for b in order:
        pltpu.make_async_copy(
            ens_hbm.at[:, columns(me, b)], arrived.at[b, members_of(me), :], fwd_recv.at[b]
        ).start()

    for load in loads:
        load.wait()
    weight[...] = jnp.sqrt(rinv[...])

    @pl.loop(0, blocks)
    def _(b):
        positions = lax.broadcasted_iota(jnp.int32, (width, slots), 0)
        selector[b] = jnp.where(positions == cell[pl.ds(b, 1), :], 1.0, 0.0).astype(BF16)

    def take_block(b):
        pltpu.make_async_copy(arrived.at[b], arrived.at[b], fwd_recv.at[b]).wait()
        alive = lax.broadcasted_iota(jnp.int32, (1, slots), 1) < count[0, b]
        root = jnp.where(alive, weight[pl.ds(b, 1), :], 0.0)
        held = observed_rows(arrived[b], selector[b], value[pl.ds(b, 1), :], root)
        rows[b] = held
        gram[b + 1] = lax.dot_general(
            held, held[:size], (((1,), (1,)), ((), ())), preferred_element_type=F32
        )

    def solve(pair):
        localized = [gram[b + 1] + localize * (gram[b] + gram[b + 2]) for b in pair]
        results = increments_of(localized, [arrived[b] for b in pair])
        for b, result in zip(pair, results):
            stage[b] = result

    def give_back(group):
        for step in range(1, groups):
            peer = lax.rem(me + step, groups)
            for b in group:
                pltpu.make_async_remote_copy(
                    src_ref=stage.at[b, members_of(peer), :],
                    dst_ref=out.at[:, columns(me, b)],
                    send_sem=ret_send,
                    recv_sem=ret_recv,
                    device_id={"mem": peer},
                    device_id_type=MESH,
                ).start()
        for b in group:
            pltpu.make_async_copy(
                stage.at[b, members_of(me), :], out.at[:, columns(me, b)], own_sem
            ).start()

    def halo(slot, peer, which):
        edge[which] = gram[slot].astype(BF16)
        return pltpu.make_async_remote_copy(
            src_ref=edge.at[which],
            dst_ref=far_edge.at[which],
            send_sem=halo_send.at[which],
            recv_sem=halo_recv.at[which],
            device_id={"mem": peer},
            device_id_type=MESH,
        )

    take_block(blocks - 1)
    upward = halo(blocks, lax.rem(me + 1, groups), 0)
    upward.start()
    take_block(0)
    downward = halo(1, lax.rem(me + groups - 1, groups), 1)
    downward.start()

    take_block(1)
    pairs = blocks // 2

    @pl.loop(0, pairs)
    def _(turn):
        b = 2 * turn + 1

        @pl.when(turn < pairs - 1)
        def _():
            @pl.loop(b + 1, jnp.minimum(b + 3, blocks - 1))
            def _(later):
                take_block(later)

        @pl.when(turn == pairs - 1)
        def _():
            upward.wait_recv()
            gram[0] = far_edge[0].astype(F32)
            downward.wait_recv()
            gram[blocks + 1] = far_edge[1].astype(F32)

        final = turn == pairs - 1
        solve([jnp.where(final, 0, b), jnp.where(final, blocks - 1, b + 1)])

        for i in range(pairs - HELD_BACK):
            @pl.when(turn == i)
            def _():
                give_back([2 * i + 1, 2 * i + 2])

    held_back = [*range(2 * (pairs - HELD_BACK) + 1, blocks), 0]
    give_back(held_back)

    upward.wait_send()
    downward.wait_send()
    share = blocks * width
    afar = pl.ds(0, (groups - 1) * share)
    pltpu.make_async_copy(out.at[:, afar], out.at[:, afar], fwd_send).wait()
    pltpu.make_async_copy(out.at[:, afar], out.at[:, afar], ret_send).wait()
    pltpu.make_async_copy(out.at[:, afar], out.at[:, afar], ret_recv).wait()
    near = pl.ds(0, share)
    pltpu.make_async_copy(out.at[:, near], out.at[:, near], own_sem).wait()


def fused(ensemble, obs_cell, obs_count, obs_value, obs_rinv):
    groups = lax.axis_size("mem")
    local, cells = ensemble.shape
    blocks, slots = obs_cell.shape[1:]
    width = cells // (groups * blocks)
    size = groups * local
    whole = pl.BlockSpec(memory_space=pltpu.VMEM)
    return pl.pallas_call(
        functools.partial(kernel, groups),
        out_shape=pltpu.VMEM(ensemble.shape, BF16),
        in_specs=[pl.BlockSpec(memory_space=pl.ANY)] * 5,
        out_specs=whole,
        scratch_shapes=[
            pltpu.VMEM((blocks, size, width), BF16),
            pltpu.VMEM((blocks, size + 16, slots), BF16),
            pltpu.VMEM((blocks + 2, size + 16, size), F32),
            pltpu.VMEM((2, size + 16, size), BF16),
            pltpu.VMEM((2, size + 16, size), BF16),
            pltpu.VMEM((blocks, width, slots), BF16),
            pltpu.VMEM((blocks, size, width), BF16),
            pltpu.VMEM((blocks, slots), F32),
            pltpu.VMEM((blocks, slots), jnp.int32),
            pltpu.SMEM(obs_count.shape, jnp.int32),
            pltpu.VMEM((blocks, slots), F32),
            pltpu.VMEM((blocks, slots), F32),
            pltpu.SemaphoreType.DMA((4,)),
            pltpu.SemaphoreType.DMA,
            pltpu.SemaphoreType.DMA,
            pltpu.SemaphoreType.DMA((blocks,)),
            pltpu.SemaphoreType.DMA,
            pltpu.SemaphoreType.DMA,
            pltpu.SemaphoreType.DMA((2,)),
            pltpu.SemaphoreType.DMA((2,)),
        ]
        + [pltpu.SemaphoreType.REGULAR] * 4,
        compiler_params=pltpu.CompilerParams(collective_id=0, has_side_effects=True),
        name="letkf",
    )(ensemble, obs_cell[0], obs_count, obs_value[0], obs_rinv[0])


def with_halo(block, sides, width):
    for axis, dim in sides:
        count = lax.axis_size(axis)
        forward = [(i, i + 1) for i in range(count - 1)]
        forward.append((count - 1, 0))
        backward = [(target, source) for source, target in forward]
        low = lax.ppermute(
            lax.slice_in_dim(block, block.shape[dim] - width, None, axis=dim), axis, forward
        )
        high = lax.ppermute(lax.slice_in_dim(block, 0, width, axis=dim), axis, backward)
        block = jnp.concatenate([low, block, high], axis=dim)
    return block


def center_blocks(members):
    values = jnp.transpose(members.astype(jnp.float32), (1, 0, 2))
    average = jnp.mean(values, axis=1)
    return (values - average[:, None, :], average)


def observe(deviation, average, cell_ids, live_counts, obs_values, inv_var):
    cell_width = deviation.shape[2]
    positions = lax.broadcasted_iota(jnp.int32, cell_ids.shape + (cell_width,), 2)
    selector = (positions == cell_ids[:, :, None]).astype(jnp.float32)
    sampled = jnp.einsum("bkc,boc->bko", deviation, selector, precision=lax.Precision.HIGHEST)
    obs_mean = jnp.einsum("bc,boc->bo", average, selector, precision=lax.Precision.HIGHEST)
    slots = lax.broadcasted_iota(jnp.int32, cell_ids.shape, 1)
    live = (slots < live_counts[:, None]).astype(jnp.float32)
    weight_root = live * jnp.sqrt(inv_var)
    upper = sampled * weight_root[:, None, :]
    lower = (weight_root * (obs_values - obs_mean))[:, None, :]
    return jnp.concatenate([upper, lower], axis=1).astype(jnp.bfloat16)


def gram_of(obs_rows):
    return jnp.einsum("bko,bjo->bkj", obs_rows, obs_rows, preferred_element_type=jnp.float32)


def batch_mm(left, right):
    return jnp.einsum("bij,bjk->bik", left, right, precision=lax.Precision.HIGHEST)


def transform_apply(localized, deviation):
    ensemble_size = deviation.shape[1]
    identity = jnp.eye(ensemble_size, dtype=jnp.float32)
    system = (ensemble_size - 1) / inflation * identity + localized[
        :, :ensemble_size, :ensemble_size
    ]
    forcing = localized[:, :ensemble_size, ensemble_size]
    bound_norm = jnp.max(jnp.sum(jnp.abs(system), axis=2), axis=1)
    approx_y = system / bound_norm[:, None, None]
    approx_z = jnp.broadcast_to(identity, system.shape)
    for iteration in range(NS_ITERS):
        update = 1.5 * identity - 0.5 * batch_mm(approx_z, approx_y)
        approx_y = batch_mm(approx_y, update)
        approx_z = batch_mm(update, approx_z)
    root_inv = approx_z / jnp.sqrt(bound_norm)[:, None, None]
    inner = jnp.einsum("bij,bj->bi", root_inv, forcing, precision=lax.Precision.HIGHEST)
    mean_weights = jnp.einsum("bij,bj->bi", root_inv, inner, precision=lax.Precision.HIGHEST)
    mixing = (
        jnp.sqrt(jnp.float32(ensemble_size - 1)) * root_inv + mean_weights[:, :, None] - identity
    )
    increment = jnp.einsum("bjc,bjk->kbc", deviation, mixing, precision=lax.Precision.HIGHEST)
    return increment.astype(jnp.bfloat16)


def on_device(ensemble, obs_cell, obs_count, obs_value, obs_rinv):
    groups = lax.axis_size("mem")
    local_members = ensemble.shape[0]
    blocks = obs_cell.shape[1]
    cell_width = ensemble.shape[1] // (groups * blocks)
    pieces = ensemble.reshape(local_members, groups, blocks, cell_width)
    arrived = lax.all_to_all(pieces, "mem", split_axis=1, concat_axis=0, tiled=True)
    deviation, average = center_blocks(arrived[:, 0])
    obs_rows = observe(deviation, average, obs_cell[0], obs_count[0], obs_value[0], obs_rinv[0])
    padded_rows = with_halo(obs_rows, (("mem", 0),), 1)
    padded = gram_of(padded_rows)
    localized = padded[1:-1] + localize * (padded[:-2] + padded[2:])
    increment = transform_apply(localized, deviation)
    ensemble_size = increment.shape[0]
    outgoing = increment.reshape(ensemble_size, 1, blocks * cell_width)
    returned = lax.all_to_all(outgoing, "mem", split_axis=0, concat_axis=1, tiled=True)
    return returned.reshape(local_members, groups * blocks * cell_width)


def by_shape(ensemble, *observations):
    groups = lax.axis_size("mem")
    local, cells = ensemble.shape
    blocks, slots = observations[0].shape[1:]
    width = cells // (groups * blocks)
    aligned = local % 16 == 0 and width % 128 == 0 and slots % 128 == 0
    aligned = aligned and (groups * local) % 128 == 0 and groups > 1 and blocks > 2 and blocks % 2 == 0
    return (fused if aligned else on_device)(ensemble, *observations)


def solution(mesh):
    placed = (
        P("mem", "blk"),
        P("blk", "mem", None),
        P("blk", "mem"),
        P("blk", "mem", None),
        P("blk", "mem", None),
    )
    return jax.shard_map(
        by_shape, mesh=mesh, in_specs=placed, out_specs=P("mem", "blk"), check_vma=False
    )
```

```python
import functools

import jax
import jax.numpy as jnp
from jax import lax
from jax.experimental import pallas as pl
from jax.experimental.pallas import tpu as pltpu
from jax.sharding import PartitionSpec as P

NS_ITERS = 4


localize = 0.5
inflation = 1.1

MESH = pl.DeviceIdType.MESH
HELD_BACK = 2
EARLY_INNER = 4
EARLY_OUTER = 3
F32 = jnp.float32
BF16 = jnp.bfloat16


def halves(x):
    high = x.astype(BF16)
    return high, (x - high.astype(F32)).astype(BF16)


def as_left(x):
    return jnp.concatenate(halves(x), axis=1)


def as_right(x):
    wide = jnp.concatenate(halves(x), axis=1)
    return jnp.concatenate([wide, wide], axis=0)


def mm(left, right):
    both = jnp.dot(left, right, preferred_element_type=F32)
    size = both.shape[1] // 2
    return both[:, :size] + both[:, size:]


def observed_rows(members, selector, values, root):
    ensemble_size = members.shape[0]
    sampled = jnp.dot(members, selector, preferred_element_type=F32)
    obs_mean = jnp.sum(sampled, axis=0, keepdims=True) * (1.0 / ensemble_size)
    upper = ((sampled - obs_mean) * root).astype(BF16)
    lower = root * (values - obs_mean)
    place = lax.broadcasted_iota(jnp.int32, (16, lower.shape[1]), 0)
    lower = jnp.where(place == 0, jnp.broadcast_to(lower, place.shape), 0.0).astype(BF16)
    return jnp.concatenate([upper, lower], axis=0)


def increments_of(localized, members):
    ensemble_size = members[0].shape[0]
    row = lax.broadcasted_iota(jnp.int32, (ensemble_size, ensemble_size), 0)
    column = lax.broadcasted_iota(jnp.int32, (ensemble_size, ensemble_size), 1)
    identity = (row == column).astype(F32)
    system = [
        (ensemble_size - 1) / inflation * identity + part[:ensemble_size] for part in localized
    ]
    bound_norm = [
        jnp.max(jnp.sum(jnp.abs(part), axis=0, keepdims=True), axis=1, keepdims=True)
        for part in system
    ]
    approx_y = [part / norm for part, norm in zip(system, bound_norm)]
    update = [1.5 * identity - 0.5 * part for part in approx_y]
    approx_z = update
    for iteration in range(1, NS_ITERS):
        approx_y = [mm(as_left(y), as_right(u)) for y, u in zip(approx_y, update)]
        left_z = [as_left(z) for z in approx_z]
        update = [
            1.5 * identity - 0.5 * mm(z, as_right(y)) for z, y in zip(left_z, approx_y)
        ]
        approx_z = [mm(z, as_right(u)) for z, u in zip(left_z, update)]
    root_inv = [z / jnp.sqrt(norm) for z, norm in zip(approx_z, bound_norm)]
    right_r = [as_right(part) for part in root_inv]
    inner = [mm(as_left(part[ensemble_size:]), r) for part, r in zip(localized, right_r)]
    mean_weights = [mm(as_left(part), r)[0:1] for part, r in zip(inner, right_r)]
    mixing = [
        jnp.sqrt(F32(ensemble_size - 1)) * part + weights - identity
        for part, weights in zip(root_inv, mean_weights)
    ]
    results = []
    for mixed, block in zip(mixing, members):
        high, low = halves(mixed)
        row_sum = jnp.sum(high.astype(F32) + low.astype(F32), axis=1, keepdims=True)
        average = jnp.sum(block.astype(F32), axis=0, keepdims=True) * (1.0 / ensemble_size)
        total = jnp.dot(
            jnp.concatenate([high, low], axis=1),
            jnp.concatenate([block, block], axis=0),
            preferred_element_type=F32,
        )
        results.append((total - row_sum * average).astype(BF16))
    return results


def fold(gram):
    size = gram.shape[1]
    half = size // 2
    top, bottom = gram[:half], pltpu.roll(gram[half:size], half, 1)
    row = lax.broadcasted_iota(jnp.int32, top.shape, 0)
    column = lax.broadcasted_iota(jnp.int32, top.shape, 1)
    left = column < half
    packed = jnp.where(left & (row > column), bottom, top)
    diagonal = jnp.sum(jnp.where(left & (row == column), bottom, 0.0), axis=0, keepdims=True)
    rest = gram[size:]
    place = lax.broadcasted_iota(jnp.int32, rest.shape, 0)
    rest = jnp.where(place == 1, jnp.broadcast_to(diagonal, rest.shape), rest)
    return jnp.concatenate([packed, rest], axis=0).astype(BF16)


def unfold(folded):
    size = folded.shape[1]
    half = size // 2
    packed, rest = folded[:half].astype(F32), folded[half:].astype(F32)
    turned = jnp.transpose(jnp.concatenate([packed, jnp.zeros_like(packed)], axis=0))
    row = lax.broadcasted_iota(jnp.int32, packed.shape, 0)
    column = lax.broadcasted_iota(jnp.int32, packed.shape, 1)
    top = jnp.where((column < half) & (row > column), turned[:half], packed)
    diagonal = jnp.broadcast_to(pltpu.roll(rest, half, 1)[1:2], packed.shape)
    lower, upper = pltpu.roll(packed, half, 1), pltpu.roll(turned[:half], half, 1)
    behind = column - half
    corner = jnp.where(row > behind, lower, jnp.where(row < behind, upper, diagonal))
    bottom = jnp.where(column < half, turned[half:], corner)
    return jnp.concatenate([top, bottom, rest], axis=0)


def kernel(
    groups,
    ens_hbm,
    cell_hbm,
    count_hbm,
    value_hbm,
    rinv_hbm,
    out,
    arrived,
    rows,
    gram,
    edge,
    far_edge,
    selector,
    stage,
    weight,
    cell,
    count,
    value,
    rinv,
    load_sem,
    own_sem,
    fwd_send,
    fwd_recv,
    ret_send,
    ret_recv,
    halo_send,
    halo_recv,
    joined,
    told,
    spread,
    complete,
):
    me = lax.axis_index("mem")
    blocks, _, width = arrived.shape
    local = ens_hbm.shape[0]
    slots = cell.shape[1]
    size = groups * local

    lanes = 2
    spots = groups // lanes
    split = groups > 2 * lanes and groups % (2 * lanes) == 0

    def central(peer):
        spot = peer // lanes
        return (spot == spots // 2 - 1) | (spot == spots // 2)

    def notify(semaphore, peer):
        pl.semaphore_signal(semaphore, inc=1, device_id={"mem": peer}, device_id_type=MESH)

    others = [lax.rem(me + step, groups) for step in range(1, groups)]
    barrier = pltpu.get_barrier_semaphore()
    if split:
        inner = central(me)
        outer = jnp.logical_not(inner)
        upper = me // lanes >= spots // 2
        lane = lax.rem(me, lanes)
        parent = (spots // 2 - 1 + upper.astype(jnp.int32)) * lanes + lane
        first = jnp.where(upper, spots // 2 + 1, 0) * lanes + lane
        children = [first + i * lanes for i in range(spots // 2 - 1)]

        def to_central(semaphore):
            for peer in others:
                pl.when(central(peer))(lambda: notify(semaphore, peer))

        def to_children(semaphore):
            for child in children:
                notify(semaphore, child)

        @pl.when(inner)
        def _():
            to_central(barrier)
            to_children(barrier)
    else:
        for peer in others:
            notify(barrier, peer)

    loads = [
        pltpu.make_async_copy(source, target, load_sem.at[i])
        for i, (source, target) in enumerate(
            ((cell_hbm, cell), (count_hbm, count), (value_hbm, value), (rinv_hbm, rinv))
        )
    ]
    for load in loads:
        load.start()
    if split:
        pl.semaphore_wait(barrier, jnp.where(inner, 2 * lanes - 1, 1))
    else:
        pl.semaphore_wait(barrier, groups - 1)

    def columns(owner, b):
        start = pl.multiple_of((owner * blocks + b) * width, width)
        return pl.ds(start, width)

    def members_of(owner):
        return pl.ds(pl.multiple_of(owner * local, local), local)

    order = [blocks - 1, *range(blocks - 1)]
    def send_to(b, peer):
        pltpu.make_async_remote_copy(
            src_ref=ens_hbm.at[:, columns(peer, b)],
            dst_ref=arrived.at[b, members_of(me), :],
            send_sem=fwd_send,
            recv_sem=fwd_recv.at[b],
            device_id={"mem": peer},
            device_id_type=MESH,
        ).start()

    def send_where(wanted, chosen):
        for b in chosen:
            for peer in others:
                pl.when(wanted(peer))(lambda: send_to(b, peer))

    def send_all(chosen):
        for b in chosen:
            for peer in others:
                send_to(b, peer)

    def beyond(peer):
        return jnp.logical_not(central(peer))

    if split:

        @pl.when(inner)
        def _():
            send_where(central, order[:EARLY_INNER])
            pl.semaphore_wait(joined, len(children))
            to_children(told)
            to_central(spread)
            pl.semaphore_wait(spread, 2 * lanes - 1)
            to_children(complete)
            send_where(beyond, order[:EARLY_INNER])
            send_all(order[EARLY_INNER:])

        @pl.when(outer)
        def _():
            notify(joined, parent)
            pl.semaphore_wait(told, 1)
            send_where(central, order[:EARLY_OUTER])
            pl.semaphore_wait(complete, 1)
            send_where(beyond, order[:EARLY_OUTER])
            send_all(order[EARLY_OUTER:])
    else:
        send_all(order)

    for b in order:
        pltpu.make_async_copy(
            ens_hbm.at[:, columns(me, b)], arrived.at[b, members_of(me), :], fwd_recv.at[b]
        ).start()

    for load in loads:
        load.wait()
    weight[...] = jnp.sqrt(rinv[...])

    @pl.loop(0, blocks)
    def _(b):
        positions = lax.broadcasted_iota(jnp.int32, (width, slots), 0)
        selector[b] = jnp.where(positions == cell[pl.ds(b, 1), :], 1.0, 0.0).astype(BF16)

    def take_block(b):
        pltpu.make_async_copy(arrived.at[b], arrived.at[b], fwd_recv.at[b]).wait()
        alive = lax.broadcasted_iota(jnp.int32, (1, slots), 1) < count[0, b]
        root = jnp.where(alive, weight[pl.ds(b, 1), :], 0.0)
        held = observed_rows(arrived[b], selector[b], value[pl.ds(b, 1), :], root)
        rows[b] = held
        gram[b + 1] = lax.dot_general(
            held, held[:size], (((1,), (1,)), ((), ())), preferred_element_type=F32
        )

    def solve(pair):
        localized = [gram[b + 1] + localize * (gram[b] + gram[b + 2]) for b in pair]
        results = increments_of(localized, [arrived[b] for b in pair])
        for b, result in zip(pair, results):
            stage[b] = result

    def give_back(group):
        for step in range(1, groups):
            peer = lax.rem(me + step, groups)
            for b in group:
                pltpu.make_async_remote_copy(
                    src_ref=stage.at[b, members_of(peer), :],
                    dst_ref=out.at[:, columns(me, b)],
                    send_sem=ret_send,
                    recv_sem=ret_recv,
                    device_id={"mem": peer},
                    device_id_type=MESH,
                ).start()
        for b in group:
            pltpu.make_async_copy(
                stage.at[b, members_of(me), :], out.at[:, columns(me, b)], own_sem
            ).start()

    def halo(slot, peer, which):
        edge[which] = fold(gram[slot])
        return pltpu.make_async_remote_copy(
            src_ref=edge.at[which],
            dst_ref=far_edge.at[which],
            send_sem=halo_send.at[which],
            recv_sem=halo_recv.at[which],
            device_id={"mem": peer},
            device_id_type=MESH,
        )

    take_block(blocks - 1)
    upward = halo(blocks, lax.rem(me + 1, groups), 0)
    upward.start()
    take_block(0)
    downward = halo(1, lax.rem(me + groups - 1, groups), 1)
    downward.start()

    take_block(1)
    pairs = blocks // 2

    @pl.loop(0, pairs)
    def _(turn):
        b = 2 * turn + 1

        @pl.when(turn < pairs - 1)
        def _():
            @pl.loop(b + 1, jnp.minimum(b + 3, blocks - 1))
            def _(later):
                take_block(later)

        @pl.when(turn == pairs - 1)
        def _():
            upward.wait_recv()
            gram[0] = unfold(far_edge[0])
            downward.wait_recv()
            gram[blocks + 1] = unfold(far_edge[1])

        final = turn == pairs - 1
        solve([jnp.where(final, 0, b), jnp.where(final, blocks - 1, b + 1)])

        for i in range(pairs - HELD_BACK):
            @pl.when(turn == i)
            def _():
                give_back([2 * i + 1, 2 * i + 2])

    held_back = [*range(2 * (pairs - HELD_BACK) + 1, blocks), 0]
    give_back(held_back)

    upward.wait_send()
    downward.wait_send()
    share = blocks * width
    afar = pl.ds(0, (groups - 1) * share)
    pltpu.make_async_copy(out.at[:, afar], out.at[:, afar], fwd_send).wait()
    pltpu.make_async_copy(out.at[:, afar], out.at[:, afar], ret_send).wait()
    pltpu.make_async_copy(out.at[:, afar], out.at[:, afar], ret_recv).wait()
    near = pl.ds(0, share)
    pltpu.make_async_copy(out.at[:, near], out.at[:, near], own_sem).wait()


def fused(ensemble, obs_cell, obs_count, obs_value, obs_rinv):
    groups = lax.axis_size("mem")
    local, cells = ensemble.shape
    blocks, slots = obs_cell.shape[1:]
    width = cells // (groups * blocks)
    size = groups * local
    whole = pl.BlockSpec(memory_space=pltpu.VMEM)
    return pl.pallas_call(
        functools.partial(kernel, groups),
        out_shape=pltpu.VMEM(ensemble.shape, BF16),
        in_specs=[pl.BlockSpec(memory_space=pl.ANY)] * 5,
        out_specs=whole,
        scratch_shapes=[
            pltpu.VMEM((blocks, size, width), BF16),
            pltpu.VMEM((blocks, size + 16, slots), BF16),
            pltpu.VMEM((blocks + 2, size + 16, size), F32),
            pltpu.VMEM((2, size // 2 + 16, size), BF16),
            pltpu.VMEM((2, size // 2 + 16, size), BF16),
            pltpu.VMEM((blocks, width, slots), BF16),
            pltpu.VMEM((blocks, size, width), BF16),
            pltpu.VMEM((blocks, slots), F32),
            pltpu.VMEM((blocks, slots), jnp.int32),
            pltpu.SMEM(obs_count.shape, jnp.int32),
            pltpu.VMEM((blocks, slots), F32),
            pltpu.VMEM((blocks, slots), F32),
            pltpu.SemaphoreType.DMA((4,)),
            pltpu.SemaphoreType.DMA,
            pltpu.SemaphoreType.DMA,
            pltpu.SemaphoreType.DMA((blocks,)),
            pltpu.SemaphoreType.DMA,
            pltpu.SemaphoreType.DMA,
            pltpu.SemaphoreType.DMA((2,)),
            pltpu.SemaphoreType.DMA((2,)),
        ]
        + [pltpu.SemaphoreType.REGULAR] * 4,
        compiler_params=pltpu.CompilerParams(collective_id=0, has_side_effects=True),
        name="letkf",
    )(ensemble, obs_cell[0], obs_count, obs_value[0], obs_rinv[0])


def with_halo(block, sides, width):
    for axis, dim in sides:
        count = lax.axis_size(axis)
        forward = [(i, i + 1) for i in range(count - 1)]
        forward.append((count - 1, 0))
        backward = [(target, source) for source, target in forward]
        low = lax.ppermute(
            lax.slice_in_dim(block, block.shape[dim] - width, None, axis=dim), axis, forward
        )
        high = lax.ppermute(lax.slice_in_dim(block, 0, width, axis=dim), axis, backward)
        block = jnp.concatenate([low, block, high], axis=dim)
    return block


def center_blocks(members):
    values = jnp.transpose(members.astype(jnp.float32), (1, 0, 2))
    average = jnp.mean(values, axis=1)
    return (values - average[:, None, :], average)


def observe(deviation, average, cell_ids, live_counts, obs_values, inv_var):
    cell_width = deviation.shape[2]
    positions = lax.broadcasted_iota(jnp.int32, cell_ids.shape + (cell_width,), 2)
    selector = (positions == cell_ids[:, :, None]).astype(jnp.float32)
    sampled = jnp.einsum("bkc,boc->bko", deviation, selector, precision=lax.Precision.HIGHEST)
    obs_mean = jnp.einsum("bc,boc->bo", average, selector, precision=lax.Precision.HIGHEST)
    slots = lax.broadcasted_iota(jnp.int32, cell_ids.shape, 1)
    live = (slots < live_counts[:, None]).astype(jnp.float32)
    weight_root = live * jnp.sqrt(inv_var)
    upper = sampled * weight_root[:, None, :]
    lower = (weight_root * (obs_values - obs_mean))[:, None, :]
    return jnp.concatenate([upper, lower], axis=1).astype(jnp.bfloat16)


def gram_of(obs_rows):
    return jnp.einsum("bko,bjo->bkj", obs_rows, obs_rows, preferred_element_type=jnp.float32)


def batch_mm(left, right):
    return jnp.einsum("bij,bjk->bik", left, right, precision=lax.Precision.HIGHEST)


def transform_apply(localized, deviation):
    ensemble_size = deviation.shape[1]
    identity = jnp.eye(ensemble_size, dtype=jnp.float32)
    system = (ensemble_size - 1) / inflation * identity + localized[
        :, :ensemble_size, :ensemble_size
    ]
    forcing = localized[:, :ensemble_size, ensemble_size]
    bound_norm = jnp.max(jnp.sum(jnp.abs(system), axis=2), axis=1)
    approx_y = system / bound_norm[:, None, None]
    approx_z = jnp.broadcast_to(identity, system.shape)
    for iteration in range(NS_ITERS):
        update = 1.5 * identity - 0.5 * batch_mm(approx_z, approx_y)
        approx_y = batch_mm(approx_y, update)
        approx_z = batch_mm(update, approx_z)
    root_inv = approx_z / jnp.sqrt(bound_norm)[:, None, None]
    inner = jnp.einsum("bij,bj->bi", root_inv, forcing, precision=lax.Precision.HIGHEST)
    mean_weights = jnp.einsum("bij,bj->bi", root_inv, inner, precision=lax.Precision.HIGHEST)
    mixing = (
        jnp.sqrt(jnp.float32(ensemble_size - 1)) * root_inv + mean_weights[:, :, None] - identity
    )
    increment = jnp.einsum("bjc,bjk->kbc", deviation, mixing, precision=lax.Precision.HIGHEST)
    return increment.astype(jnp.bfloat16)


def on_device(ensemble, obs_cell, obs_count, obs_value, obs_rinv):
    groups = lax.axis_size("mem")
    local_members = ensemble.shape[0]
    blocks = obs_cell.shape[1]
    cell_width = ensemble.shape[1] // (groups * blocks)
    pieces = ensemble.reshape(local_members, groups, blocks, cell_width)
    arrived = lax.all_to_all(pieces, "mem", split_axis=1, concat_axis=0, tiled=True)
    deviation, average = center_blocks(arrived[:, 0])
    obs_rows = observe(deviation, average, obs_cell[0], obs_count[0], obs_value[0], obs_rinv[0])
    padded_rows = with_halo(obs_rows, (("mem", 0),), 1)
    padded = gram_of(padded_rows)
    localized = padded[1:-1] + localize * (padded[:-2] + padded[2:])
    increment = transform_apply(localized, deviation)
    ensemble_size = increment.shape[0]
    outgoing = increment.reshape(ensemble_size, 1, blocks * cell_width)
    returned = lax.all_to_all(outgoing, "mem", split_axis=0, concat_axis=1, tiled=True)
    return returned.reshape(local_members, groups * blocks * cell_width)


def by_shape(ensemble, *observations):
    groups = lax.axis_size("mem")
    local, cells = ensemble.shape
    blocks, slots = observations[0].shape[1:]
    width = cells // (groups * blocks)
    aligned = local % 16 == 0 and width % 128 == 0 and slots % 128 == 0
    aligned = aligned and (groups * local) % 128 == 0 and groups > 1 and blocks > 2 and blocks % 2 == 0
    return (fused if aligned else on_device)(ensemble, *observations)


def solution(mesh):
    placed = (
        P("mem", "blk"),
        P("blk", "mem", None),
        P("blk", "mem"),
        P("blk", "mem", None),
        P("blk", "mem", None),
    )
    return jax.shard_map(
        by_shape, mesh=mesh, in_specs=placed, out_specs=P("mem", "blk"), check_vma=False
    )
```

```python
import functools

import jax
import jax.numpy as jnp
from jax import lax
from jax.experimental import pallas as pl
from jax.experimental.pallas import tpu as pltpu
from jax.sharding import PartitionSpec as P

NS_ITERS = 4


localize = 0.5
inflation = 1.1

MESH = pl.DeviceIdType.MESH
HELD_BACK = 2
EARLY_INNER = 4
EARLY_OUTER = 3
F32 = jnp.float32
BF16 = jnp.bfloat16


def halves(x):
    high = x.astype(BF16)
    return high, (x - high.astype(F32)).astype(BF16)


def as_left(x):
    return jnp.concatenate(halves(x), axis=1)


def as_right(x):
    wide = jnp.concatenate(halves(x), axis=1)
    return jnp.concatenate([wide, wide], axis=0)


def mm(left, right):
    both = jnp.dot(left, right, preferred_element_type=F32)
    size = both.shape[1] // 2
    return both[:, :size] + both[:, size:]


def observed_rows(members, selector, values, root):
    ensemble_size = members.shape[0]
    sampled = jnp.dot(members, selector, preferred_element_type=F32)
    obs_mean = jnp.sum(sampled, axis=0, keepdims=True) * (1.0 / ensemble_size)
    upper = ((sampled - obs_mean) * root).astype(BF16)
    lower = root * (values - obs_mean)
    place = lax.broadcasted_iota(jnp.int32, (16, lower.shape[1]), 0)
    lower = jnp.where(place == 0, jnp.broadcast_to(lower, place.shape), 0.0).astype(BF16)
    return jnp.concatenate([upper, lower], axis=0)


def increments_of(localized, members):
    ensemble_size = members[0].shape[0]
    row = lax.broadcasted_iota(jnp.int32, (ensemble_size, ensemble_size), 0)
    column = lax.broadcasted_iota(jnp.int32, (ensemble_size, ensemble_size), 1)
    identity = (row == column).astype(F32)
    system = [
        (ensemble_size - 1) / inflation * identity + part[:ensemble_size] for part in localized
    ]
    bound_norm = [
        jnp.max(jnp.sum(jnp.abs(part), axis=0, keepdims=True), axis=1, keepdims=True)
        for part in system
    ]
    approx_y = [part / norm for part, norm in zip(system, bound_norm)]
    update = [1.5 * identity - 0.5 * part for part in approx_y]
    approx_z = update
    for iteration in range(1, NS_ITERS):
        approx_y = [mm(as_left(y), as_right(u)) for y, u in zip(approx_y, update)]
        left_z = [as_left(z) for z in approx_z]
        update = [
            1.5 * identity - 0.5 * mm(z, as_right(y)) for z, y in zip(left_z, approx_y)
        ]
        approx_z = [mm(z, as_right(u)) for z, u in zip(left_z, update)]
    root_inv = [z / jnp.sqrt(norm) for z, norm in zip(approx_z, bound_norm)]
    right_r = [as_right(part) for part in root_inv]
    inner = [mm(as_left(part[ensemble_size:]), r) for part, r in zip(localized, right_r)]
    mean_weights = [mm(as_left(part), r)[0:1] for part, r in zip(inner, right_r)]
    mixing = [
        jnp.sqrt(F32(ensemble_size - 1)) * part + weights - identity
        for part, weights in zip(root_inv, mean_weights)
    ]
    results = []
    for mixed, block in zip(mixing, members):
        high, low = halves(mixed)
        row_sum = jnp.sum(high.astype(F32) + low.astype(F32), axis=1, keepdims=True)
        average = jnp.sum(block.astype(F32), axis=0, keepdims=True) * (1.0 / ensemble_size)
        total = jnp.dot(
            jnp.concatenate([high, low], axis=1),
            jnp.concatenate([block, block], axis=0),
            preferred_element_type=F32,
        )
        results.append((total - row_sum * average).astype(BF16))
    return results


def fold(gram):
    size = gram.shape[1]
    half = size // 2
    top, bottom = gram[:half], pltpu.roll(gram[half:size], half, 1)
    row = lax.broadcasted_iota(jnp.int32, top.shape, 0)
    column = lax.broadcasted_iota(jnp.int32, top.shape, 1)
    left = column < half
    packed = jnp.where(left & (row > column), bottom, top)
    diagonal = jnp.sum(jnp.where(left & (row == column), bottom, 0.0), axis=0, keepdims=True)
    rest = gram[size:]
    place = lax.broadcasted_iota(jnp.int32, rest.shape, 0)
    rest = jnp.where(place == 1, jnp.broadcast_to(diagonal, rest.shape), rest)
    return jnp.concatenate([packed, rest], axis=0).astype(BF16)


def unfold(folded):
    size = folded.shape[1]
    half = size // 2
    packed, rest = folded[:half].astype(F32), folded[half:].astype(F32)
    turned = jnp.transpose(jnp.concatenate([packed, jnp.zeros_like(packed)], axis=0))
    row = lax.broadcasted_iota(jnp.int32, packed.shape, 0)
    column = lax.broadcasted_iota(jnp.int32, packed.shape, 1)
    top = jnp.where((column < half) & (row > column), turned[:half], packed)
    diagonal = jnp.broadcast_to(pltpu.roll(rest, half, 1)[1:2], packed.shape)
    lower, upper = pltpu.roll(packed, half, 1), pltpu.roll(turned[:half], half, 1)
    behind = column - half
    corner = jnp.where(row > behind, lower, jnp.where(row < behind, upper, diagonal))
    bottom = jnp.where(column < half, turned[half:], corner)
    return jnp.concatenate([top, bottom, rest], axis=0)


def kernel(
    groups,
    ens_hbm,
    cell_hbm,
    count_hbm,
    value_hbm,
    rinv_hbm,
    out,
    arrived,
    rows,
    gram,
    edge,
    far_edge,
    selector,
    stage,
    weight,
    cell,
    count,
    value,
    rinv,
    load_sem,
    own_sem,
    fwd_send,
    fwd_recv,
    ret_send,
    ret_recv,
    halo_send,
    halo_recv,
    joined,
    told,
    spread,
    complete,
):
    me = lax.axis_index("mem")
    blocks, _, width = arrived.shape
    local = ens_hbm.shape[0]
    slots = cell.shape[1]
    size = groups * local

    lanes = 2
    spots = groups // lanes
    split = groups == 4 * lanes

    def central(peer):
        spot = peer // lanes
        return (spot == spots // 2 - 1) | (spot == spots // 2)

    def notify(semaphore, peer):
        pl.semaphore_signal(semaphore, inc=1, device_id={"mem": peer}, device_id_type=MESH)

    others = [lax.rem(me + step, groups) for step in range(1, groups)]
    barrier = pltpu.get_barrier_semaphore()
    if split:
        inner = central(me)
        outer = jnp.logical_not(inner)
        spot, lane = me // lanes, lax.rem(me, lanes)
        upper = spot >= spots // 2
        turn_lane = 1 - 2 * lane
        across = (spots - 1 - spot) * lanes + lane
        slant, beside = across + turn_lane, me + turn_lane
        parent = jnp.where(upper, spots // 2, spots // 2 - 1) * lanes + lane
        child = jnp.where(upper, spots - 1, 0) * lanes + lane
        opposite = jnp.where(upper, spots // 2 - 1, spots // 2) * lanes + lane
        near_mid = [parent, parent + turn_lane]
        far_mid = [opposite, opposite + turn_lane]
        middle = (across, beside, slant)

        def to_central(semaphore):
            for peer in middle:
                notify(semaphore, peer)

        def to_children(semaphore):
            notify(semaphore, child)

        @pl.when(inner)
        def _():
            to_central(barrier)
            to_children(barrier)
    else:
        for peer in others:
            notify(barrier, peer)

    loads = [
        pltpu.make_async_copy(source, target, load_sem.at[i])
        for i, (source, target) in enumerate(
            ((cell_hbm, cell), (count_hbm, count), (value_hbm, value), (rinv_hbm, rinv))
        )
    ]
    for load in loads:
        load.start()
    if split:
        pl.semaphore_wait(barrier, jnp.where(inner, 2 * lanes - 1, 1))
    else:
        pl.semaphore_wait(barrier, groups - 1)

    def columns(owner, b):
        start = pl.multiple_of((owner * blocks + b) * width, width)
        return pl.ds(start, width)

    def members_of(owner):
        return pl.ds(pl.multiple_of(owner * local, local), local)

    order = [blocks - 1, *range(blocks - 1)]
    def send_to(b, peer):
        pltpu.make_async_remote_copy(
            src_ref=ens_hbm.at[:, columns(peer, b)],
            dst_ref=arrived.at[b, members_of(me), :],
            send_sem=fwd_send,
            recv_sem=fwd_recv.at[b],
            device_id={"mem": peer},
            device_id_type=MESH,
        ).start()

    def send_where(wanted, chosen):
        for b in chosen:
            for peer in others:
                pl.when(wanted(peer))(lambda: send_to(b, peer))

    def send_to_some(peers, chosen):
        for b in chosen:
            for peer in peers:
                send_to(b, peer)

    def send_all(chosen):
        for b in chosen:
            for peer in others:
                send_to(b, peer)

    def beyond(peer):
        return jnp.logical_not(central(peer))

    if split:

        @pl.when(inner)
        def _():
            send_to_some(middle, order[:EARLY_INNER])
            pl.semaphore_wait(joined, 1)
            to_children(told)
            to_central(spread)
            pl.semaphore_wait(spread, 2 * lanes - 1)
            to_children(complete)
            send_where(beyond, order[:EARLY_INNER])
            send_all(order[EARLY_INNER:])

        @pl.when(outer)
        def _():
            notify(joined, parent)
            pl.semaphore_wait(told, 1)
            send_to_some(far_mid + near_mid, order[:EARLY_OUTER])
            pl.semaphore_wait(complete, 1)
            send_to_some((beside, across, slant), order[:EARLY_OUTER])
            send_all(order[EARLY_OUTER:])
    else:
        send_all(order)

    for b in order:
        pltpu.make_async_copy(
            ens_hbm.at[:, columns(me, b)], arrived.at[b, members_of(me), :], fwd_recv.at[b]
        ).start()

    for load in loads:
        load.wait()
    weight[...] = jnp.sqrt(rinv[...])

    @pl.loop(0, blocks)
    def _(b):
        positions = lax.broadcasted_iota(jnp.int32, (width, slots), 0)
        selector[b] = jnp.where(positions == cell[pl.ds(b, 1), :], 1.0, 0.0).astype(BF16)

    def take_block(b):
        pltpu.make_async_copy(arrived.at[b], arrived.at[b], fwd_recv.at[b]).wait()
        alive = lax.broadcasted_iota(jnp.int32, (1, slots), 1) < count[0, b]
        root = jnp.where(alive, weight[pl.ds(b, 1), :], 0.0)
        held = observed_rows(arrived[b], selector[b], value[pl.ds(b, 1), :], root)
        rows[b] = held
        gram[b + 1] = lax.dot_general(
            held, held[:size], (((1,), (1,)), ((), ())), preferred_element_type=F32
        )

    def solve(pair):
        localized = [gram[b + 1] + localize * (gram[b] + gram[b + 2]) for b in pair]
        results = increments_of(localized, [arrived[b] for b in pair])
        for b, result in zip(pair, results):
            stage[b] = result

    def give_back(group):
        for step in range(1, groups):
            peer = lax.rem(me + step, groups)
            for b in group:
                pltpu.make_async_remote_copy(
                    src_ref=stage.at[b, members_of(peer), :],
                    dst_ref=out.at[:, columns(me, b)],
                    send_sem=ret_send,
                    recv_sem=ret_recv,
                    device_id={"mem": peer},
                    device_id_type=MESH,
                ).start()
        for b in group:
            pltpu.make_async_copy(
                stage.at[b, members_of(me), :], out.at[:, columns(me, b)], own_sem
            ).start()

    def halo(slot, peer, which):
        edge[which] = fold(gram[slot])
        return pltpu.make_async_remote_copy(
            src_ref=edge.at[which],
            dst_ref=far_edge.at[which],
            send_sem=halo_send.at[which],
            recv_sem=halo_recv.at[which],
            device_id={"mem": peer},
            device_id_type=MESH,
        )

    take_block(blocks - 1)
    upward = halo(blocks, lax.rem(me + 1, groups), 0)
    upward.start()
    take_block(0)
    downward = halo(1, lax.rem(me + groups - 1, groups), 1)
    downward.start()

    take_block(1)
    pairs = blocks // 2

    @pl.loop(0, pairs)
    def _(turn):
        b = 2 * turn + 1

        @pl.when(turn < pairs - 1)
        def _():
            @pl.loop(b + 1, jnp.minimum(b + 3, blocks - 1))
            def _(later):
                take_block(later)

        @pl.when(turn == pairs - 1)
        def _():
            upward.wait_recv()
            gram[0] = unfold(far_edge[0])
            downward.wait_recv()
            gram[blocks + 1] = unfold(far_edge[1])

        final = turn == pairs - 1
        solve([jnp.where(final, 0, b), jnp.where(final, blocks - 1, b + 1)])

        for i in range(pairs - HELD_BACK):
            @pl.when(turn == i)
            def _():
                give_back([2 * i + 1, 2 * i + 2])

    held_back = [*range(2 * (pairs - HELD_BACK) + 1, blocks), 0]
    give_back(held_back)

    upward.wait_send()
    downward.wait_send()
    share = blocks * width
    afar = pl.ds(0, (groups - 1) * share)
    pltpu.make_async_copy(out.at[:, afar], out.at[:, afar], fwd_send).wait()
    pltpu.make_async_copy(out.at[:, afar], out.at[:, afar], ret_send).wait()
    pltpu.make_async_copy(out.at[:, afar], out.at[:, afar], ret_recv).wait()
    near = pl.ds(0, share)
    pltpu.make_async_copy(out.at[:, near], out.at[:, near], own_sem).wait()


def fused(ensemble, obs_cell, obs_count, obs_value, obs_rinv):
    groups = lax.axis_size("mem")
    local, cells = ensemble.shape
    blocks, slots = obs_cell.shape[1:]
    width = cells // (groups * blocks)
    size = groups * local
    whole = pl.BlockSpec(memory_space=pltpu.VMEM)
    return pl.pallas_call(
        functools.partial(kernel, groups),
        out_shape=pltpu.VMEM(ensemble.shape, BF16),
        in_specs=[pl.BlockSpec(memory_space=pl.ANY)] * 5,
        out_specs=whole,
        scratch_shapes=[
            pltpu.VMEM((blocks, size, width), BF16),
            pltpu.VMEM((blocks, size + 16, slots), BF16),
            pltpu.VMEM((blocks + 2, size + 16, size), F32),
            pltpu.VMEM((2, size // 2 + 16, size), BF16),
            pltpu.VMEM((2, size // 2 + 16, size), BF16),
            pltpu.VMEM((blocks, width, slots), BF16),
            pltpu.VMEM((blocks, size, width), BF16),
            pltpu.VMEM((blocks, slots), F32),
            pltpu.VMEM((blocks, slots), jnp.int32),
            pltpu.SMEM(obs_count.shape, jnp.int32),
            pltpu.VMEM((blocks, slots), F32),
            pltpu.VMEM((blocks, slots), F32),
            pltpu.SemaphoreType.DMA((4,)),
            pltpu.SemaphoreType.DMA,
            pltpu.SemaphoreType.DMA,
            pltpu.SemaphoreType.DMA((blocks,)),
            pltpu.SemaphoreType.DMA,
            pltpu.SemaphoreType.DMA,
            pltpu.SemaphoreType.DMA((2,)),
            pltpu.SemaphoreType.DMA((2,)),
        ]
        + [pltpu.SemaphoreType.REGULAR] * 4,
        compiler_params=pltpu.CompilerParams(collective_id=0, has_side_effects=True),
        name="letkf",
    )(ensemble, obs_cell[0], obs_count, obs_value[0], obs_rinv[0])


def with_halo(block, sides, width):
    for axis, dim in sides:
        count = lax.axis_size(axis)
        forward = [(i, i + 1) for i in range(count - 1)]
        forward.append((count - 1, 0))
        backward = [(target, source) for source, target in forward]
        low = lax.ppermute(
            lax.slice_in_dim(block, block.shape[dim] - width, None, axis=dim), axis, forward
        )
        high = lax.ppermute(lax.slice_in_dim(block, 0, width, axis=dim), axis, backward)
        block = jnp.concatenate([low, block, high], axis=dim)
    return block


def center_blocks(members):
    values = jnp.transpose(members.astype(jnp.float32), (1, 0, 2))
    average = jnp.mean(values, axis=1)
    return (values - average[:, None, :], average)


def observe(deviation, average, cell_ids, live_counts, obs_values, inv_var):
    cell_width = deviation.shape[2]
    positions = lax.broadcasted_iota(jnp.int32, cell_ids.shape + (cell_width,), 2)
    selector = (positions == cell_ids[:, :, None]).astype(jnp.float32)
    sampled = jnp.einsum("bkc,boc->bko", deviation, selector, precision=lax.Precision.HIGHEST)
    obs_mean = jnp.einsum("bc,boc->bo", average, selector, precision=lax.Precision.HIGHEST)
    slots = lax.broadcasted_iota(jnp.int32, cell_ids.shape, 1)
    live = (slots < live_counts[:, None]).astype(jnp.float32)
    weight_root = live * jnp.sqrt(inv_var)
    upper = sampled * weight_root[:, None, :]
    lower = (weight_root * (obs_values - obs_mean))[:, None, :]
    return jnp.concatenate([upper, lower], axis=1).astype(jnp.bfloat16)


def gram_of(obs_rows):
    return jnp.einsum("bko,bjo->bkj", obs_rows, obs_rows, preferred_element_type=jnp.float32)


def batch_mm(left, right):
    return jnp.einsum("bij,bjk->bik", left, right, precision=lax.Precision.HIGHEST)


def transform_apply(localized, deviation):
    ensemble_size = deviation.shape[1]
    identity = jnp.eye(ensemble_size, dtype=jnp.float32)
    system = (ensemble_size - 1) / inflation * identity + localized[
        :, :ensemble_size, :ensemble_size
    ]
    forcing = localized[:, :ensemble_size, ensemble_size]
    bound_norm = jnp.max(jnp.sum(jnp.abs(system), axis=2), axis=1)
    approx_y = system / bound_norm[:, None, None]
    approx_z = jnp.broadcast_to(identity, system.shape)
    for iteration in range(NS_ITERS):
        update = 1.5 * identity - 0.5 * batch_mm(approx_z, approx_y)
        approx_y = batch_mm(approx_y, update)
        approx_z = batch_mm(update, approx_z)
    root_inv = approx_z / jnp.sqrt(bound_norm)[:, None, None]
    inner = jnp.einsum("bij,bj->bi", root_inv, forcing, precision=lax.Precision.HIGHEST)
    mean_weights = jnp.einsum("bij,bj->bi", root_inv, inner, precision=lax.Precision.HIGHEST)
    mixing = (
        jnp.sqrt(jnp.float32(ensemble_size - 1)) * root_inv + mean_weights[:, :, None] - identity
    )
    increment = jnp.einsum("bjc,bjk->kbc", deviation, mixing, precision=lax.Precision.HIGHEST)
    return increment.astype(jnp.bfloat16)


def on_device(ensemble, obs_cell, obs_count, obs_value, obs_rinv):
    groups = lax.axis_size("mem")
    local_members = ensemble.shape[0]
    blocks = obs_cell.shape[1]
    cell_width = ensemble.shape[1] // (groups * blocks)
    pieces = ensemble.reshape(local_members, groups, blocks, cell_width)
    arrived = lax.all_to_all(pieces, "mem", split_axis=1, concat_axis=0, tiled=True)
    deviation, average = center_blocks(arrived[:, 0])
    obs_rows = observe(deviation, average, obs_cell[0], obs_count[0], obs_value[0], obs_rinv[0])
    padded_rows = with_halo(obs_rows, (("mem", 0),), 1)
    padded = gram_of(padded_rows)
    localized = padded[1:-1] + localize * (padded[:-2] + padded[2:])
    increment = transform_apply(localized, deviation)
    ensemble_size = increment.shape[0]
    outgoing = increment.reshape(ensemble_size, 1, blocks * cell_width)
    returned = lax.all_to_all(outgoing, "mem", split_axis=0, concat_axis=1, tiled=True)
    return returned.reshape(local_members, groups * blocks * cell_width)


def by_shape(ensemble, *observations):
    groups = lax.axis_size("mem")
    local, cells = ensemble.shape
    blocks, slots = observations[0].shape[1:]
    width = cells // (groups * blocks)
    aligned = local % 16 == 0 and width % 128 == 0 and slots % 128 == 0
    aligned = aligned and (groups * local) % 128 == 0 and groups > 1 and blocks > 2 and blocks % 2 == 0
    return (fused if aligned else on_device)(ensemble, *observations)


def solution(mesh):
    placed = (
        P("mem", "blk"),
        P("blk", "mem", None),
        P("blk", "mem"),
        P("blk", "mem", None),
        P("blk", "mem", None),
    )
    return jax.shard_map(
        by_shape, mesh=mesh, in_specs=placed, out_specs=P("mem", "blk"), check_vma=False
    )
```

```python
import functools

import jax
import jax.numpy as jnp
from jax import lax
from jax.experimental import pallas as pl
from jax.experimental.pallas import tpu as pltpu
from jax.sharding import PartitionSpec as P

NS_ITERS = 4


localize = 0.5
inflation = 1.1

MESH = pl.DeviceIdType.MESH
HELD_BACK = 2
EARLY_INNER = 4
EARLY_OUTER = 3
F32 = jnp.float32
BF16 = jnp.bfloat16


def halves(x):
    high = x.astype(BF16)
    return high, (x - high.astype(F32)).astype(BF16)


def as_left(x):
    return jnp.concatenate(halves(x), axis=1)


def as_right(x):
    wide = jnp.concatenate(halves(x), axis=1)
    return jnp.concatenate([wide, wide], axis=0)


def mm(left, right):
    both = jnp.dot(left, right, preferred_element_type=F32)
    size = both.shape[1] // 2
    return both[:, :size] + both[:, size:]


def observed_rows(members, selector, values, root):
    ensemble_size = members.shape[0]
    sampled = jnp.dot(members, selector, preferred_element_type=F32)
    obs_mean = jnp.sum(sampled, axis=0, keepdims=True) * (1.0 / ensemble_size)
    upper = ((sampled - obs_mean) * root).astype(BF16)
    lower = root * (values - obs_mean)
    place = lax.broadcasted_iota(jnp.int32, (16, lower.shape[1]), 0)
    lower = jnp.where(place == 0, jnp.broadcast_to(lower, place.shape), 0.0).astype(BF16)
    return jnp.concatenate([upper, lower], axis=0)


def increments_of(localized, members):
    ensemble_size = members[0].shape[0]
    row = lax.broadcasted_iota(jnp.int32, (ensemble_size, ensemble_size), 0)
    column = lax.broadcasted_iota(jnp.int32, (ensemble_size, ensemble_size), 1)
    identity = (row == column).astype(F32)
    system = [
        (ensemble_size - 1) / inflation * identity + part[:ensemble_size] for part in localized
    ]
    bound_norm = [
        jnp.max(jnp.sum(jnp.abs(part), axis=0, keepdims=True), axis=1, keepdims=True)
        for part in system
    ]
    approx_y = [part / norm for part, norm in zip(system, bound_norm)]
    update = [1.5 * identity - 0.5 * part for part in approx_y]
    approx_z = update
    for iteration in range(1, NS_ITERS):
        approx_y = [mm(as_left(y), as_right(u)) for y, u in zip(approx_y, update)]
        left_z = [as_left(z) for z in approx_z]
        update = [
            1.5 * identity - 0.5 * mm(z, as_right(y)) for z, y in zip(left_z, approx_y)
        ]
        approx_z = [mm(z, as_right(u)) for z, u in zip(left_z, update)]
    root_inv = [z / jnp.sqrt(norm) for z, norm in zip(approx_z, bound_norm)]
    right_r = [as_right(part) for part in root_inv]
    inner = [mm(as_left(part[ensemble_size:]), r) for part, r in zip(localized, right_r)]
    mean_weights = [mm(as_left(part), r)[0:1] for part, r in zip(inner, right_r)]
    mixing = [
        jnp.sqrt(F32(ensemble_size - 1)) * part + weights - identity
        for part, weights in zip(root_inv, mean_weights)
    ]
    results = []
    for mixed, block in zip(mixing, members):
        high, low = halves(mixed)
        row_sum = jnp.sum(high.astype(F32) + low.astype(F32), axis=1, keepdims=True)
        average = jnp.sum(block.astype(F32), axis=0, keepdims=True) * (1.0 / ensemble_size)
        total = jnp.dot(
            jnp.concatenate([high, low], axis=1),
            jnp.concatenate([block, block], axis=0),
            preferred_element_type=F32,
        )
        results.append((total - row_sum * average).astype(BF16))
    return results


def fold(gram):
    size = gram.shape[1]
    half = size // 2
    top, bottom = gram[:half], pltpu.roll(gram[half:size], half, 1)
    row = lax.broadcasted_iota(jnp.int32, top.shape, 0)
    column = lax.broadcasted_iota(jnp.int32, top.shape, 1)
    left = column < half
    packed = jnp.where(left & (row > column), bottom, top)
    diagonal = jnp.sum(jnp.where(left & (row == column), bottom, 0.0), axis=0, keepdims=True)
    rest = gram[size:]
    place = lax.broadcasted_iota(jnp.int32, rest.shape, 0)
    rest = jnp.where(place == 1, jnp.broadcast_to(diagonal, rest.shape), rest)
    return jnp.concatenate([packed, rest], axis=0).astype(BF16)


def unfold(folded):
    size = folded.shape[1]
    half = size // 2
    packed, rest = folded[:half].astype(F32), folded[half:].astype(F32)
    turned = jnp.transpose(jnp.concatenate([packed, jnp.zeros_like(packed)], axis=0))
    row = lax.broadcasted_iota(jnp.int32, packed.shape, 0)
    column = lax.broadcasted_iota(jnp.int32, packed.shape, 1)
    top = jnp.where((column < half) & (row > column), turned[:half], packed)
    diagonal = jnp.broadcast_to(pltpu.roll(rest, half, 1)[1:2], packed.shape)
    lower, upper = pltpu.roll(packed, half, 1), pltpu.roll(turned[:half], half, 1)
    behind = column - half
    corner = jnp.where(row > behind, lower, jnp.where(row < behind, upper, diagonal))
    bottom = jnp.where(column < half, turned[half:], corner)
    return jnp.concatenate([top, bottom, rest], axis=0)


def kernel(
    groups,
    ens_hbm,
    cell_hbm,
    count_hbm,
    value_hbm,
    rinv_hbm,
    out,
    arrived,
    rows,
    gram,
    edge,
    far_edge,
    selector,
    stage,
    weight,
    cell,
    count,
    value,
    rinv,
    load_sem,
    own_sem,
    fwd_send,
    fwd_recv,
    ret_send,
    ret_recv,
    halo_send,
    halo_recv,
    joined,
    told,
    spread,
    complete,
):
    me = lax.axis_index("mem")
    odd = lax.rem(lax.axis_index("blk"), 2) == 1
    blocks, _, width = arrived.shape
    local = ens_hbm.shape[0]
    slots = cell.shape[1]
    size = groups * local

    lanes = 2
    spots = groups // lanes
    split = groups == 4 * lanes

    def central(peer):
        spot = peer // lanes
        return (spot == spots // 2 - 1) | (spot == spots // 2)

    def notify(semaphore, peer):
        pl.semaphore_signal(semaphore, inc=1, device_id={"mem": peer}, device_id_type=MESH)

    others = [lax.rem(me + step, groups) for step in range(1, groups)]
    barrier = pltpu.get_barrier_semaphore()
    if split:
        inner = central(me)
        outer = jnp.logical_not(inner)
        spot, lane = me // lanes, lax.rem(me, lanes)
        upper = spot >= spots // 2
        turn_lane = 1 - 2 * lane
        across = (spots - 1 - spot) * lanes + lane
        slant, beside = across + turn_lane, me + turn_lane
        parent = jnp.where(upper, spots // 2, spots // 2 - 1) * lanes + lane
        child = jnp.where(upper, spots - 1, 0) * lanes + lane
        opposite = jnp.where(upper, spots // 2 - 1, spots // 2) * lanes + lane
        near_mid = [parent, parent + turn_lane]
        far_mid = [opposite, opposite + turn_lane]
        middle = (across, beside, slant)

        def to_central(semaphore):
            for peer in middle:
                notify(semaphore, peer)

        def to_children(semaphore):
            notify(semaphore, child)

        @pl.when(inner)
        def _():
            to_central(barrier)
            to_children(barrier)
    else:
        for peer in others:
            notify(barrier, peer)

    loads = [
        pltpu.make_async_copy(source, target, load_sem.at[i])
        for i, (source, target) in enumerate(
            ((cell_hbm, cell), (count_hbm, count), (value_hbm, value), (rinv_hbm, rinv))
        )
    ]
    for load in loads:
        load.start()
    if split:
        pl.semaphore_wait(barrier, jnp.where(inner, 2 * lanes - 1, 1))
    else:
        pl.semaphore_wait(barrier, groups - 1)

    def columns(owner, b):
        start = pl.multiple_of((owner * blocks + b) * width, width)
        return pl.ds(start, width)

    def members_of(owner):
        return pl.ds(pl.multiple_of(owner * local, local), local)

    order = [blocks - 1, *range(blocks - 1)]
    def send_to(b, peer):
        pltpu.make_async_remote_copy(
            src_ref=ens_hbm.at[:, columns(peer, b)],
            dst_ref=arrived.at[b, members_of(me), :],
            send_sem=fwd_send,
            recv_sem=fwd_recv.at[b],
            device_id={"mem": peer},
            device_id_type=MESH,
        ).start()

    def send_where(wanted, chosen):
        for b in chosen:
            for peer in others:
                pl.when(wanted(peer))(lambda: send_to(b, peer))

    def send_to_some(peers, chosen):
        for b in chosen:
            for peer in peers:
                send_to(b, peer)

    def send_all(chosen):
        for b in chosen:
            for peer in others:
                send_to(b, peer)

    def beyond(peer):
        return jnp.logical_not(central(peer))

    if split:

        @pl.when(inner)
        def _():
            send_to_some(middle, order[:EARLY_INNER])
            pl.semaphore_wait(joined, 1)
            to_children(told)
            to_central(spread)
            pl.semaphore_wait(spread, 2 * lanes - 1)
            to_children(complete)
            send_where(beyond, order[:EARLY_INNER])
            send_all(order[EARLY_INNER:6])

        @pl.when(outer)
        def _():
            notify(joined, parent)
            pl.semaphore_wait(told, 1)
            send_to_some(far_mid + near_mid, order[:EARLY_OUTER])
            pl.semaphore_wait(complete, 1)
            send_to_some((beside, across, slant), order[:EARLY_OUTER])
            send_all(order[EARLY_OUTER:6])
    else:
        send_all(order[:6])

    @pl.when(jnp.logical_not(odd))
    def _():
        send_all(order[6:])

    for b in order:
        pltpu.make_async_copy(
            ens_hbm.at[:, columns(me, b)], arrived.at[b, members_of(me), :], fwd_recv.at[b]
        ).start()

    for load in loads:
        load.wait()
    weight[...] = jnp.sqrt(rinv[...])

    @pl.loop(0, blocks)
    def _(b):
        positions = lax.broadcasted_iota(jnp.int32, (width, slots), 0)
        selector[b] = jnp.where(positions == cell[pl.ds(b, 1), :], 1.0, 0.0).astype(BF16)

    def take_block(b):
        pltpu.make_async_copy(arrived.at[b], arrived.at[b], fwd_recv.at[b]).wait()
        alive = lax.broadcasted_iota(jnp.int32, (1, slots), 1) < count[0, b]
        root = jnp.where(alive, weight[pl.ds(b, 1), :], 0.0)
        held = observed_rows(arrived[b], selector[b], value[pl.ds(b, 1), :], root)
        rows[b] = held
        gram[b + 1] = lax.dot_general(
            held, held[:size], (((1,), (1,)), ((), ())), preferred_element_type=F32
        )

    def solve(pair):
        localized = [gram[b + 1] + localize * (gram[b] + gram[b + 2]) for b in pair]
        results = increments_of(localized, [arrived[b] for b in pair])
        for b, result in zip(pair, results):
            stage[b] = result

    def give_back(group):
        for step in range(1, groups):
            peer = lax.rem(me + step, groups)
            for b in group:
                pltpu.make_async_remote_copy(
                    src_ref=stage.at[b, members_of(peer), :],
                    dst_ref=out.at[:, columns(me, b)],
                    send_sem=ret_send,
                    recv_sem=ret_recv,
                    device_id={"mem": peer},
                    device_id_type=MESH,
                ).start()
        for b in group:
            pltpu.make_async_copy(
                stage.at[b, members_of(me), :], out.at[:, columns(me, b)], own_sem
            ).start()

    def halo(slot, peer, which):
        edge[which] = fold(gram[slot])
        return pltpu.make_async_remote_copy(
            src_ref=edge.at[which],
            dst_ref=far_edge.at[which],
            send_sem=halo_send.at[which],
            recv_sem=halo_recv.at[which],
            device_id={"mem": peer},
            device_id_type=MESH,
        )

    take_block(blocks - 1)

    @pl.when(odd)
    def _():
        send_all(order[6:])

    upward = halo(blocks, lax.rem(me + 1, groups), 0)
    upward.start()
    take_block(0)
    downward = halo(1, lax.rem(me + groups - 1, groups), 1)
    downward.start()

    take_block(1)
    pairs = blocks // 2

    @pl.loop(0, pairs)
    def _(turn):
        b = 2 * turn + 1

        @pl.when(turn < pairs - 1)
        def _():
            @pl.loop(b + 1, jnp.minimum(b + 3, blocks - 1))
            def _(later):
                take_block(later)

        @pl.when(turn == pairs - 1)
        def _():
            upward.wait_recv()
            gram[0] = unfold(far_edge[0])
            downward.wait_recv()
            gram[blocks + 1] = unfold(far_edge[1])

        final = turn == pairs - 1
        solve([jnp.where(final, 0, b), jnp.where(final, blocks - 1, b + 1)])

        for i in range(pairs - HELD_BACK):
            @pl.when(turn == i)
            def _():
                give_back([2 * i + 1, 2 * i + 2])

    held_back = [*range(2 * (pairs - HELD_BACK) + 1, blocks), 0]
    give_back(held_back)

    upward.wait_send()
    downward.wait_send()
    share = blocks * width
    afar = pl.ds(0, (groups - 1) * share)
    pltpu.make_async_copy(out.at[:, afar], out.at[:, afar], fwd_send).wait()
    pltpu.make_async_copy(out.at[:, afar], out.at[:, afar], ret_send).wait()
    pltpu.make_async_copy(out.at[:, afar], out.at[:, afar], ret_recv).wait()
    near = pl.ds(0, share)
    pltpu.make_async_copy(out.at[:, near], out.at[:, near], own_sem).wait()


def fused(ensemble, obs_cell, obs_count, obs_value, obs_rinv):
    groups = lax.axis_size("mem")
    local, cells = ensemble.shape
    blocks, slots = obs_cell.shape[1:]
    width = cells // (groups * blocks)
    size = groups * local
    whole = pl.BlockSpec(memory_space=pltpu.VMEM)
    return pl.pallas_call(
        functools.partial(kernel, groups),
        out_shape=pltpu.VMEM(ensemble.shape, BF16),
        in_specs=[pl.BlockSpec(memory_space=pl.ANY)] * 5,
        out_specs=whole,
        scratch_shapes=[
            pltpu.VMEM((blocks, size, width), BF16),
            pltpu.VMEM((blocks, size + 16, slots), BF16),
            pltpu.VMEM((blocks + 2, size + 16, size), F32),
            pltpu.VMEM((2, size // 2 + 16, size), BF16),
            pltpu.VMEM((2, size // 2 + 16, size), BF16),
            pltpu.VMEM((blocks, width, slots), BF16),
            pltpu.VMEM((blocks, size, width), BF16),
            pltpu.VMEM((blocks, slots), F32),
            pltpu.VMEM((blocks, slots), jnp.int32),
            pltpu.SMEM(obs_count.shape, jnp.int32),
            pltpu.VMEM((blocks, slots), F32),
            pltpu.VMEM((blocks, slots), F32),
            pltpu.SemaphoreType.DMA((4,)),
            pltpu.SemaphoreType.DMA,
            pltpu.SemaphoreType.DMA,
            pltpu.SemaphoreType.DMA((blocks,)),
            pltpu.SemaphoreType.DMA,
            pltpu.SemaphoreType.DMA,
            pltpu.SemaphoreType.DMA((2,)),
            pltpu.SemaphoreType.DMA((2,)),
        ]
        + [pltpu.SemaphoreType.REGULAR] * 4,
        compiler_params=pltpu.CompilerParams(collective_id=0, has_side_effects=True),
        name="letkf",
    )(ensemble, obs_cell[0], obs_count, obs_value[0], obs_rinv[0])


def with_halo(block, sides, width):
    for axis, dim in sides:
        count = lax.axis_size(axis)
        forward = [(i, i + 1) for i in range(count - 1)]
        forward.append((count - 1, 0))
        backward = [(target, source) for source, target in forward]
        low = lax.ppermute(
            lax.slice_in_dim(block, block.shape[dim] - width, None, axis=dim), axis, forward
        )
        high = lax.ppermute(lax.slice_in_dim(block, 0, width, axis=dim), axis, backward)
        block = jnp.concatenate([low, block, high], axis=dim)
    return block


def center_blocks(members):
    values = jnp.transpose(members.astype(jnp.float32), (1, 0, 2))
    average = jnp.mean(values, axis=1)
    return (values - average[:, None, :], average)


def observe(deviation, average, cell_ids, live_counts, obs_values, inv_var):
    cell_width = deviation.shape[2]
    positions = lax.broadcasted_iota(jnp.int32, cell_ids.shape + (cell_width,), 2)
    selector = (positions == cell_ids[:, :, None]).astype(jnp.float32)
    sampled = jnp.einsum("bkc,boc->bko", deviation, selector, precision=lax.Precision.HIGHEST)
    obs_mean = jnp.einsum("bc,boc->bo", average, selector, precision=lax.Precision.HIGHEST)
    slots = lax.broadcasted_iota(jnp.int32, cell_ids.shape, 1)
    live = (slots < live_counts[:, None]).astype(jnp.float32)
    weight_root = live * jnp.sqrt(inv_var)
    upper = sampled * weight_root[:, None, :]
    lower = (weight_root * (obs_values - obs_mean))[:, None, :]
    return jnp.concatenate([upper, lower], axis=1).astype(jnp.bfloat16)


def gram_of(obs_rows):
    return jnp.einsum("bko,bjo->bkj", obs_rows, obs_rows, preferred_element_type=jnp.float32)


def batch_mm(left, right):
    return jnp.einsum("bij,bjk->bik", left, right, precision=lax.Precision.HIGHEST)


def transform_apply(localized, deviation):
    ensemble_size = deviation.shape[1]
    identity = jnp.eye(ensemble_size, dtype=jnp.float32)
    system = (ensemble_size - 1) / inflation * identity + localized[
        :, :ensemble_size, :ensemble_size
    ]
    forcing = localized[:, :ensemble_size, ensemble_size]
    bound_norm = jnp.max(jnp.sum(jnp.abs(system), axis=2), axis=1)
    approx_y = system / bound_norm[:, None, None]
    approx_z = jnp.broadcast_to(identity, system.shape)
    for iteration in range(NS_ITERS):
        update = 1.5 * identity - 0.5 * batch_mm(approx_z, approx_y)
        approx_y = batch_mm(approx_y, update)
        approx_z = batch_mm(update, approx_z)
    root_inv = approx_z / jnp.sqrt(bound_norm)[:, None, None]
    inner = jnp.einsum("bij,bj->bi", root_inv, forcing, precision=lax.Precision.HIGHEST)
    mean_weights = jnp.einsum("bij,bj->bi", root_inv, inner, precision=lax.Precision.HIGHEST)
    mixing = (
        jnp.sqrt(jnp.float32(ensemble_size - 1)) * root_inv + mean_weights[:, :, None] - identity
    )
    increment = jnp.einsum("bjc,bjk->kbc", deviation, mixing, precision=lax.Precision.HIGHEST)
    return increment.astype(jnp.bfloat16)


def on_device(ensemble, obs_cell, obs_count, obs_value, obs_rinv):
    groups = lax.axis_size("mem")
    local_members = ensemble.shape[0]
    blocks = obs_cell.shape[1]
    cell_width = ensemble.shape[1] // (groups * blocks)
    pieces = ensemble.reshape(local_members, groups, blocks, cell_width)
    arrived = lax.all_to_all(pieces, "mem", split_axis=1, concat_axis=0, tiled=True)
    deviation, average = center_blocks(arrived[:, 0])
    obs_rows = observe(deviation, average, obs_cell[0], obs_count[0], obs_value[0], obs_rinv[0])
    padded_rows = with_halo(obs_rows, (("mem", 0),), 1)
    padded = gram_of(padded_rows)
    localized = padded[1:-1] + localize * (padded[:-2] + padded[2:])
    increment = transform_apply(localized, deviation)
    ensemble_size = increment.shape[0]
    outgoing = increment.reshape(ensemble_size, 1, blocks * cell_width)
    returned = lax.all_to_all(outgoing, "mem", split_axis=0, concat_axis=1, tiled=True)
    return returned.reshape(local_members, groups * blocks * cell_width)


def by_shape(ensemble, *observations):
    groups = lax.axis_size("mem")
    local, cells = ensemble.shape
    blocks, slots = observations[0].shape[1:]
    width = cells // (groups * blocks)
    aligned = local % 16 == 0 and width % 128 == 0 and slots % 128 == 0
    aligned = aligned and (groups * local) % 128 == 0 and groups > 1 and blocks > 2 and blocks % 2 == 0
    return (fused if aligned else on_device)(ensemble, *observations)


def solution(mesh):
    placed = (
        P("mem", "blk"),
        P("blk", "mem", None),
        P("blk", "mem"),
        P("blk", "mem", None),
        P("blk", "mem", None),
    )
    return jax.shard_map(
        by_shape, mesh=mesh, in_specs=placed, out_specs=P("mem", "blk"), check_vma=False
    )
```
